32 devices in a mesh: lon: 8 (over y, x, core), lat: 4 (over z).
Axes of the slice: x: 2, y: 2, z: 4, core: 2. Of those that a mesh axis runs over, the one named last changes fastest.
Arguments:
- fields: bfloat16 [32, 256, 256], P('lat', 'lon'), may hold values from -6 to 6
- norm_lon: float32 [256], replicated, may hold values from 0.25 to 1.75
- query_lon: bfloat16 [256, 256], replicated, may hold values from -0.375 to 0.375
- key_lon: bfloat16 [256, 256], replicated, may hold values from -0.375 to 0.375
- value_lon: bfloat16 [256, 256], replicated, may hold values from -0.375 to 0.375
- out_lon: bfloat16 [256, 256], replicated, may hold values from -0.375 to 0.375
- temp_lon: float32 [8], replicated, may hold values from 0.5 to 12
- bias_lon: float32 [8], replicated, may hold values from -2 to 2
- norm_lat: float32 [256], replicated, may hold values from 0.25 to 1.75
- query_lat: bfloat16 [256, 256], replicated, may hold values from -0.375 to 0.375
- key_lat: bfloat16 [256, 256], replicated, may hold values from -0.375 to 0.375
- value_lat: bfloat16 [256, 256], replicated, may hold values from -0.375 to 0.375
- out_lat: bfloat16 [256, 256], replicated, may hold values from -0.375 to 0.375
- temp_lat: float32 [8], replicated, may hold values from 0.5 to 12
- bias_lat: float32 [8], replicated, may hold values from -4 to 0
- norm_mlp: float32 [256], replicated, may hold values from 0.25 to 1.75
- w_gate: bfloat16 [256, 1024], replicated, may hold values from -0.375 to 0.375
- w_up: bfloat16 [256, 1024], replicated, may hold values from -0.375 to 0.375
- w_down: bfloat16 [1024, 256], replicated, may hold values from -0.1875 to 0.1875
Outputs:
- updated: bfloat16 [32, 256, 256], P('lat', 'lon')
The draws below stay inside these ranges and needn't reach their ends.
All inputs are finite; a program needn't handle non-finite values.
Results may differ from the reference program's by a relative error of at most 0.018.
The reference program's roundings to bfloat16 on the way count: a program that leaves them out, or rounds other values in their place, can miss the bound.
Values may be sent and summed in bfloat16 or wider, within the bound.
A program may use at most 64 MiB of HBM per device.

```python
import math
import jax
import jax.numpy as jnp
from jax import lax

D = 256
HEADS = 8
FF = 1024
HEAD = 32
LON_DEV = 32
NLON = 256
NLAT = 32


def block_scale(rng, shape, cuts, least, high):
    def one(dim, parts):
        steps = jax.random.uniform(jax.random.fold_in(jax.random.fold_in(rng, 6), dim), (parts,), jnp.float32, least / len(cuts), high / len(cuts))
        return jnp.repeat(jnp.exp(steps), shape[dim] // parts).reshape((-1,) + (1,) * (len(shape) - dim - 1))

    loudness = one(*cuts[0])
    for cut in cuts[1:]:
        loudness = loudness * one(*cut)
    return loudness


def scatter_about(own_key, extent, scale, reach, shards=(), kind=jnp.bfloat16):
    entries = jax.random.normal(own_key, extent, jnp.float32) * scale
    if len(shards) > 0:
        entries = block_scale(own_key, extent, shards, -0.22, 0.18) * entries
    return jnp.clip(entries, min=-reach, max=reach).astype(kind)


def setup_inputs(seed: int = 0) -> dict:
    seeds = jax.random.split(jax.random.key(seed), 20)
    fields = scatter_about(seeds[0], (NLAT, NLON, D), 1.0, 6.0, ((0, 4), (1, 8)))
    norm_lon = jnp.clip(1.0 + 0.15 * jax.random.normal(seeds[1], (D,), jnp.float32), 0.25, 1.75)
    query_lon = scatter_about(seeds[2], (D, D), D ** -0.5, 0.375)
    key_lon = scatter_about(seeds[3], (D, D), D ** -0.5, 0.375)
    value_lon = scatter_about(seeds[4], (D, D), D ** -0.5, 0.375)
    out_lon = scatter_about(seeds[5], (D, D), D ** -0.5, 0.375)
    temp_lon = jnp.clip(jnp.exp(jax.random.uniform(seeds[6], (HEADS,), jnp.float32, math.log(0.5), math.log(12.0))), 0.5, 12.0)
    bias_lon = jnp.clip(jax.random.uniform(seeds[7], (HEADS,), jnp.float32, -2.0, 2.0), -2.0, 2.0)
    norm_lat = jnp.clip(1.0 + 0.15 * jax.random.normal(seeds[8], (D,), jnp.float32), 0.25, 1.75)
    query_lat = scatter_about(seeds[9], (D, D), D ** -0.5, 0.375)
    key_lat = scatter_about(seeds[10], (D, D), D ** -0.5, 0.375)
    value_lat = scatter_about(seeds[11], (D, D), D ** -0.5, 0.375)
    out_lat = scatter_about(seeds[12], (D, D), D ** -0.5, 0.375)
    temp_lat = jnp.clip(jnp.exp(jax.random.uniform(seeds[13], (HEADS,), jnp.float32, math.log(0.5), math.log(12.0))), 0.5, 12.0)
    bias_lat = jnp.clip(jax.random.uniform(seeds[14], (HEADS,), jnp.float32, -4.0, 0.0), -4.0, 0.0)
    norm_mlp = jnp.clip(1.0 + 0.15 * jax.random.normal(seeds[15], (D,), jnp.float32), 0.25, 1.75)
    w_gate = scatter_about(seeds[16], (D, FF), D ** -0.5, 0.375)
    w_up = scatter_about(seeds[17], (D, FF), D ** -0.5, 0.375)
    w_down = scatter_about(seeds[18], (FF, D), FF ** -0.5, 0.1875)
    return dict(fields=fields, norm_lon=norm_lon, query_lon=query_lon, key_lon=key_lon, value_lon=value_lon, out_lon=out_lon, temp_lon=temp_lon, bias_lon=bias_lon, norm_lat=norm_lat, query_lat=query_lat, key_lat=key_lat, value_lat=value_lat, out_lat=out_lat, temp_lat=temp_lat, bias_lat=bias_lat, norm_mlp=norm_mlp, w_gate=w_gate, w_up=w_up, w_down=w_down)


def normalize(values, gain):
    wide = values.astype(jnp.float32)
    factor = lax.rsqrt(lax.optimization_barrier(jnp.mean(wide * wide, axis=-1, keepdims=True)) + 1e-06)
    return (wide * factor * gain).astype(jnp.bfloat16)

def project(values, weight):
    return jnp.dot(values, weight, preferred_element_type=jnp.float32).astype(jnp.bfloat16)

def attend_lat(queries, keys, values, temp, bias):
    count, cols, depth = queries.shape
    heads = temp.shape[0]
    size = depth // heads
    qh = queries.reshape(count, cols, heads, size).astype(jnp.float32)
    kh = keys.reshape(count, cols, heads, size).astype(jnp.float32)
    vh = values.reshape(count, cols, heads, size).astype(jnp.float32)
    scores = jnp.einsum('ichd,jchd->chij', qh, kh)
    place = jnp.arange(count, dtype=jnp.int32)
    spread = jnp.abs(place[:, None] - place[None, :]).astype(jnp.float32) / count
    scores = scores * (temp / math.sqrt(size))[None, :, None, None] + bias[None, :, None, None] * spread[None, None]
    expo = jnp.exp(scores - lax.optimization_barrier(jnp.max(scores, axis=-1, keepdims=True)))
    denom = lax.optimization_barrier(jnp.sum(expo, axis=-1))
    mixed = jnp.einsum('chij,jchd->ichd', expo.astype(jnp.bfloat16).astype(jnp.float32), vh)
    mixed = mixed / jnp.transpose(denom, (2, 0, 1))[..., None]
    return mixed.astype(jnp.bfloat16).reshape(count, cols, depth)

def reference(fields, norm_lon, query_lon, key_lon, value_lon, out_lon, temp_lon, bias_lon, norm_lat, query_lat, key_lat, value_lat, out_lat, temp_lat, bias_lat, norm_mlp, w_gate, w_up, w_down):
    resid = fields.astype(jnp.float32)
    normed = normalize(resid, norm_lon)
    queries = project(normed, query_lon)
    keys = project(normed, key_lon)
    values = project(normed, value_lon)
    place = jnp.arange(NLON, dtype=jnp.int32)
    angle = (place[:, None] - place[None, :]).astype(jnp.float32) * (2.0 * math.pi / NLON)
    wave = jnp.cos(angle)

    def lon_row(items):
        qr, kr, vr = items
        qh = qr.reshape(NLON, HEADS, HEAD).astype(jnp.float32)
        kh = kr.reshape(NLON, HEADS, HEAD).astype(jnp.float32)
        vh = vr.reshape(NLON, HEADS, HEAD).astype(jnp.float32)
        scores = jnp.einsum('ihd,jhd->hij', qh, kh)
        scores = scores * (temp_lon / math.sqrt(HEAD))[:, None, None] + bias_lon[:, None, None] * wave[None]
        expo = jnp.exp(scores - lax.optimization_barrier(jnp.max(scores, axis=-1, keepdims=True)))
        denom = lax.optimization_barrier(jnp.sum(expo, axis=-1))
        mixed = jnp.einsum('hij,jhd->ihd', expo.astype(jnp.bfloat16).astype(jnp.float32), vh)
        mixed = mixed / jnp.transpose(denom)[..., None]
        return mixed.astype(jnp.bfloat16).reshape(NLON, D)
    attended = lax.map(lon_row, (queries, keys, values))
    first = resid + jnp.dot(attended, out_lon, preferred_element_type=jnp.float32)
    normed_lat = normalize(first, norm_lat)
    blocks = NLON // LON_DEV

    def split(values_in):
        return jnp.transpose(values_in.reshape(NLAT, blocks, LON_DEV, D), (1, 0, 2, 3))
    q2 = split(project(normed_lat, query_lat))
    k2 = split(project(normed_lat, key_lat))
    v2 = split(project(normed_lat, value_lat))
    mixed_lat = lax.map(lambda items: attend_lat(items[0], items[1], items[2], temp_lat, bias_lat), (q2, k2, v2))
    mixed_lat = jnp.transpose(mixed_lat, (1, 0, 2, 3)).reshape(NLAT, NLON, D)
    second = first + jnp.dot(mixed_lat, out_lat, preferred_element_type=jnp.float32)
    normed_mlp = normalize(second, norm_mlp)
    gate = jnp.dot(normed_mlp, w_gate, preferred_element_type=jnp.float32)
    upper = jnp.dot(normed_mlp, w_up, preferred_element_type=jnp.float32)
    hidden = (jax.nn.silu(gate) * upper).astype(jnp.bfloat16)
    return (second + jnp.dot(hidden, w_down, preferred_element_type=jnp.float32)).astype(jnp.bfloat16)
```

```python
import math

import jax
import jax.numpy as jnp
import functools
import numpy as np
from jax import lax
from jax.experimental import pallas as pl
from jax.experimental.pallas import tpu as pltpu
from jax.sharding import PartitionSpec as P


def normalize(values, gain):
    factor = lax.rsqrt(jnp.mean(values * values, axis=-1, keepdims=True) + 1e-06)
    return (values * factor * gain).astype(jnp.bfloat16)


def project(values, weight):
    return jnp.dot(values, weight, preferred_element_type=jnp.float32).astype(jnp.bfloat16)


def attend_lat(queries, keys, values, temp, bias):
    count, cols, depth = queries.shape
    heads = temp.shape[0]
    size = depth // heads
    qh = queries.reshape(count, cols, heads, size)
    kh = keys.reshape(count, cols, heads, size)
    vh = values.reshape(count, cols, heads, size)
    scores = jnp.einsum("ichd,jchd->chij", qh, kh, preferred_element_type=jnp.float32)
    place = jnp.arange(count, dtype=jnp.int32)
    spread = jnp.abs(place[:, None] - place[None, :]).astype(jnp.float32) / count
    scores = (
        scores * (temp / math.sqrt(size))[None, :, None, None]
        + bias[None, :, None, None] * spread[None, None]
    )
    expo = jnp.exp(scores - jnp.max(scores, axis=-1, keepdims=True))
    denom = jnp.sum(expo, axis=-1)
    mixed = jnp.einsum(
        "chij,jchd->ichd", expo.astype(jnp.bfloat16), vh, preferred_element_type=jnp.float32
    )
    mixed = mixed / jnp.transpose(denom, (2, 0, 1))[..., None]
    return mixed.astype(jnp.bfloat16).reshape(count, cols, depth)


def body(
    fields,
    norm_lon,
    query_lon,
    key_lon,
    value_lon,
    out_lon,
    temp_lon,
    bias_lon,
    norm_lat,
    query_lat,
    key_lat,
    value_lat,
    out_lat,
    temp_lat,
    bias_lat,
    norm_mlp,
    w_gate,
    w_up,
    w_down,
):
    rows, width, depth = fields.shape
    heads = temp_lon.shape[0]
    size = depth // heads
    total_lon = width * lax.axis_size("lon")
    resid = fields.astype(jnp.float32)
    normed = normalize(resid, norm_lon)
    scale_lon = temp_lon / math.sqrt(size)
    query_place = lax.axis_index("lon") * width + jnp.arange(width, dtype=jnp.int32)
    queries = project(normed, query_lon).reshape(rows, width, heads, size)
    piece = lax.all_gather(normed, "lon", axis=1, tiled=True)
    keys = project(piece, key_lon)
    count = keys.shape[1]
    key_place = jnp.arange(count, dtype=jnp.int32)
    angle = (query_place[:, None] - key_place[None, :]).astype(jnp.float32) * (
        2.0 * math.pi / total_lon
    )
    wave = jnp.cos(angle)

    def one_row(items):
        query_row, key_row, value_row, peak, total, accum = items
        key_heads = key_row.reshape(count, heads, size)
        value_heads = value_row.reshape(count, heads, size)
        scores = jnp.einsum(
            "ihd,jhd->hij", query_row, key_heads, preferred_element_type=jnp.float32
        )
        scores = scores * scale_lon[:, None, None] + bias_lon[:, None, None] * wave[None]
        fresh = jnp.maximum(peak, jnp.max(scores, axis=-1))
        shrink = jnp.exp(peak - fresh)
        expo = jnp.exp(scores - fresh[..., None])
        total = total * shrink + jnp.sum(expo, axis=-1)
        mixed = jnp.einsum(
            "hij,jhd->ihd",
            expo.astype(jnp.bfloat16),
            value_heads,
            preferred_element_type=jnp.float32,
        )
        accum = accum.reshape(width, heads, size) * jnp.transpose(shrink)[:, :, None] + mixed
        return (fresh, total, accum.reshape(width, depth))

    peak = jnp.full((rows, heads, width), -1e30, jnp.float32)
    total = jnp.zeros((rows, heads, width), jnp.float32)
    accum = jnp.zeros((rows, width, depth), jnp.float32)
    peak, total, accum = lax.map(
        one_row, (queries, keys, project(piece, value_lon), peak, total, accum)
    )
    attended = accum.reshape(rows, width, heads, size) / jnp.transpose(total, (0, 2, 1))[..., None]
    attended = attended.astype(jnp.bfloat16).reshape(rows, width, depth)
    first = resid + jnp.dot(attended, out_lon, preferred_element_type=jnp.float32)
    normed_lat = normalize(first, norm_lat)
    query_col = project(normed_lat, query_lat)
    key_col = project(normed_lat, key_lat)
    value_col = project(normed_lat, value_lat)
    query_col, key_col, value_col = (
        lax.all_to_all(query_col, "lat", split_axis=1, concat_axis=0, tiled=True),
        lax.all_to_all(key_col, "lat", split_axis=1, concat_axis=0, tiled=True),
        lax.all_to_all(value_col, "lat", split_axis=1, concat_axis=0, tiled=True),
    )
    mixed_lat = attend_lat(query_col, key_col, value_col, temp_lat, bias_lat)
    returned = lax.all_to_all(mixed_lat, "lat", split_axis=0, concat_axis=1, tiled=True)
    second = first + jnp.dot(returned, out_lat, preferred_element_type=jnp.float32)
    normed_mlp = normalize(second, norm_mlp)
    gate = jnp.dot(normed_mlp, w_gate, preferred_element_type=jnp.float32)
    upper = jnp.dot(normed_mlp, w_up, preferred_element_type=jnp.float32)
    hidden = (jax.nn.silu(gate) * upper).astype(jnp.bfloat16)
    return (second + jnp.dot(hidden, w_down, preferred_element_type=jnp.float32)).astype(
        jnp.bfloat16
    )


NT = (((1,), (1,)), ((), ()))
MESH = pl.DeviceIdType.MESH
F32 = jnp.float32
BF16 = jnp.bfloat16
LANES = 128
LOG2E = math.log2(math.e)


def mm(a, b):
    return jnp.dot(a, b, preferred_element_type=F32)


def mm_nt(a, b):
    return lax.dot_general(a, b, NT, preferred_element_type=F32)


def iota(shape, dim):
    return lax.broadcasted_iota(jnp.int32, shape, dim)


def partner(me, step, n):
    if n & (n - 1):
        return lax.rem(me + step, n)
    bits = [b for b in range(n.bit_length()) if step >> b & 1]
    return sum((1 - 2 * lax.rem(me // (1 << b), 2)) * (1 << b) for b in bits) + me


def far_first(n):
    return sorted(range(1, n), key=lambda step: -(2 * (step >> 1).bit_count() + (step & 1)))


def split_pairs(values, odd):
    high = values.astype(BF16).astype(F32)
    return jnp.where(odd, values - high, high)


class Attention:
    def __init__(self, keys, extra_keys, queries_t, extras, values_t, size):
        self.keys, self.extra_keys, self.queries_t, self.extras = keys, extra_keys, queries_t, extras
        self.values_t, self.size = values_t, size
        self.stages = (self.scores, self.weights, self.mixed, self.divided)
        self.held = {}

    def scores(self, b, h):
        size = self.size
        per_group = LANES // size
        group = h // per_group
        blank = jnp.zeros((size, LANES), BF16)
        pieces = []
        for g in range(group * per_group, (group + 1) * per_group):
            rows = self.queries_t[g * size:(g + 1) * size, b * LANES:(b + 1) * LANES]
            pieces.append(jnp.concatenate([rows if g == h else blank, rows if g == h + 1 else blank], axis=1))
        pieces.append(jnp.concatenate([self.extras(b, h), self.extras(b, h + 1)], axis=1))
        left = jnp.concatenate([self.keys[:, group * LANES:(group + 1) * LANES], self.extra_keys], axis=1)
        self.held[b, h] = mm(left, jnp.concatenate(pieces, axis=0))

    def weights(self, b, h):
        scores = self.held[b, h]
        self.held[b, h] = jnp.exp2((scores - jnp.max(scores, axis=0, keepdims=True)).astype(BF16))

    def mixed(self, b, h):
        ones = jnp.ones((16, self.keys.shape[0]), BF16)
        left = jnp.concatenate([self.values_t[h * self.size:(h + 2) * self.size, :], ones], axis=0)
        self.held[b, h] = mm(left, self.held[b, h])

    def divided(self, b, h):
        size = self.size
        mixed = self.held[b, h]
        share = 1.0 / mixed[2 * size:2 * size + 1, :]
        self.held[b, h] = jnp.concatenate(
            [mixed[:size, :LANES] * share[:, :LANES], mixed[size:2 * size, LANES:] * share[:, LANES:]], axis=0
        )

    def taken(self, b, heads):
        return jnp.concatenate([self.held.pop((b, h)) for h in range(0, heads, 2)], axis=0).T


def staggered(stages, units, after):
    for step in range(len(units) + len(stages) - 1):
        for s, stage in enumerate(stages):
            if 0 <= step - s < len(units):
                stage(*units[step - s])
        if step >= len(stages) - 1:
            after(*units[step - len(stages) + 1])


def block_kernel(
    n_lon, n_lat, rows, width, depth, heads,
    fields_h, gain_lon_h, gain_lat_h, gain_mlp_h, temp_lon_h, bias_lon_h, temp_lat_h, bias_lat_h,
    ktab_h, qtab_h, wq1_h, wk1_h, wv1_h, wo1_h, wq2_h, wk2_h, wv2_h, wo2_h, wg_h, wu_h, wd_h,
    out,
    fields, gain_lon, gain_lat, gain_mlp, temp_lon, bias_lon, temp_lat, bias_lat,
    ktab, qtab, wq1, wk1, wv1, wo1, wq2, wk2, wv2, wo2, wg, wu, wd,
    norm_out, norm_in, field_out, field_in, att_out, att_in, upd_out,
    wqv1, wqv2, extra1, extra2, onehot,
    local_sem, s1, r1, s2, r2, s3, r3, s4, r4, line_sem, plane_sem,
):
    me_lon = lax.axis_index("lon")
    me_lat = lax.axis_index("lat")
    total = n_lon * n_lat
    size = depth // heads
    cols = width // n_lat
    count = n_lat * rows
    cells = rows * width
    half = n_lat // 2
    side = me_lat // half
    own = lax.rem(me_lat, half)
    far = (1 - side) * half

    def lat_at(slot):
        return lax.rem(slot + far, n_lat)

    loads = {}

    def load(name, src, dst):
        loads[name] = pltpu.make_async_copy(src, dst, local_sem.at[len(loads)])
        loads[name].start()

    load("fields", fields_h, fields)
    load("gain_lon", gain_lon_h, gain_lon)
    barrier = pltpu.get_barrier_semaphore()
    order = far_first(n_lon)

    def signal_plane(sem):
        for step in order:
            pl.semaphore_signal(
                sem, inc=1, device_id=(partner(me_lon, step, n_lon), me_lat), device_id_type=MESH
            )

    def signal_line(sem):
        @pl.when(me_lat > 0)
        def _():
            pl.semaphore_signal(sem, inc=1, device_id=(me_lon, me_lat - 1), device_id_type=MESH)

        @pl.when(me_lat < n_lat - 1)
        def _():
            pl.semaphore_signal(sem, inc=1, device_id=(me_lon, me_lat + 1), device_id_type=MESH)

    beside = jnp.minimum(me_lat, 1) + jnp.minimum(n_lat - 1 - me_lat, 1)
    signal_plane(barrier)
    signal_line(barrier)
    load("ktab0", ktab_h.at[pl.ds(far, half)], ktab.at[pl.ds(0, half)])
    load("ktab1", ktab_h.at[pl.ds(half - far, half)], ktab.at[pl.ds(half, half)])
    load("qtab0", qtab_h.at[pl.ds(1 - side, 1)], qtab.at[pl.ds(0, 1)])
    load("qtab1", qtab_h.at[pl.ds(side, 1)], qtab.at[pl.ds(1, 1)])
    for name, src, dst in [
        ("wq1", wq1_h, wq1), ("wk1", wk1_h, wk1), ("wv1", wv1_h, wv1), ("temp_lon", temp_lon_h, temp_lon),
        ("bias_lon", bias_lon_h, bias_lon), ("temp_lat", temp_lat_h, temp_lat), ("bias_lat", bias_lat_h, bias_lat),
        ("wo1", wo1_h, wo1), ("wq2", wq2_h, wq2), ("wk2", wk2_h, wk2), ("wv2", wv2_h, wv2), ("wo2", wo2_h, wo2),
        ("wg", wg_h, wg), ("wu", wu_h, wu), ("wd", wd_h, wd), ("gain_lat", gain_lat_h, gain_lat),
        ("gain_mlp", gain_mlp_h, gain_mlp),
    ]:
        load(name, src, dst)

    loads["fields"].wait()
    loads["gain_lon"].wait()
    wide = fields[...].astype(F32)
    factor = lax.rsqrt(jnp.mean(wide * wide, axis=-1, keepdims=True) + 1e-06)
    scaled = (wide * factor * gain_lon[...][None]).reshape(rows, n_lat, cols, depth).astype(BF16)
    pieces = wide.reshape(rows, n_lat, cols, depth).astype(BF16)
    for a in range(n_lat):
        norm_out[:, pl.ds(lax.rem(a + n_lat - far, n_lat), 1)] = scaled[:, a:a + 1]
        field_out[a] = pieces[:, a]

    pl.semaphore_wait(barrier, n_lon - 1 + beside)

    def my_cols(ref):
        return ref.at[:, pl.ds(pl.multiple_of(me_lat * cols, cols), cols), :]

    def send_norm(step):
        peer = partner(me_lon, step, n_lon)
        return pltpu.make_async_remote_copy(
            src_ref=norm_out.at[peer], dst_ref=norm_in.at[:, me_lon],
            send_sem=s1.at[0], recv_sem=r1.at[0], device_id=(peer, me_lat), device_id_type=MESH,
        )

    def send_field(peer):
        slot = lax.rem(me_lat + n_lat - (1 - peer // half) * half, n_lat)
        return pltpu.make_async_remote_copy(
            src_ref=field_out.at[peer], dst_ref=field_in.at[slot], send_sem=s2.at[0],
            recv_sem=r2.at[0], device_id=(me_lon, peer), device_id_type=MESH,
        )

    def send_fields(hop):
        @pl.when(me_lat >= hop)
        def _():
            send_field(me_lat - hop).start()

        @pl.when(me_lat + hop < n_lat)
        def _():
            send_field(me_lat + hop).start()

    def whole(src, dst, sends, recvs):
        return pltpu.make_async_remote_copy(
            src_ref=src, dst_ref=dst, send_sem=sends, recv_sem=recvs,
            device_id=(me_lon, me_lat), device_id_type=MESH,
        )

    for step in order:
        send_norm(step).start()
    for hop in range(1, n_lat):
        if hop > 1:
            pl.semaphore_wait(line_sem.at[hop - 1], beside)
        if hop < n_lat - 1:
            signal_line(line_sem.at[hop])
        send_fields(hop)
    signal_plane(plane_sem)
    norm_in[:, pl.ds(me_lon, 1)] = norm_out[pl.ds(me_lon, 1)].reshape(n_lat, 1, cols, depth)
    field_in[pl.ds(half + own, 1)] = field_out[pl.ds(me_lat, 1)]

    for name in ("wq1", "wk1", "wv1", "temp_lon", "bias_lon", "temp_lat", "bias_lat", "ktab0", "ktab1", "qtab0", "qtab1"):
        loads[name].wait()
    wqv1[:depth] = wq1[...].T
    wqv1[depth:] = wv1[...].T
    shape = (16, LANES)
    odd = lax.rem(iota(shape, 0), 2) == 1
    for h in range(heads):
        for b in range(2):
            extra1[b, h] = split_pairs(bias_lon[:, h:h + 1] * LOG2E * qtab[b], odd).astype(BF16)
    lanes = iota((cells, LANES), 1)
    slot = iota((cells, LANES), 0) // cols
    col = lax.rem(iota((cells, LANES), 0), cols)
    hot = (lanes == slot) | (lanes == slot + count) | (lanes == col + 2 * count)
    onehot[...] = jnp.where(hot, 1.0, 0.0).astype(BF16)
    shape = (LANES, LANES)
    line = iota(shape, 0)
    for b in range(2):
        cell = iota(shape, 1) + b * LANES
        here = lax.rem(line + far * rows, count)
        there = lax.rem(cell // cols + far * rows, count)
        apart = jnp.abs(here - there).astype(F32) / count
        fence = jnp.where(line - 2 * count == lax.rem(cell, cols), 0.0, -1e30)
        for h in range(heads):
            term = split_pairs(bias_lat[:, h:h + 1] * LOG2E * apart, line >= count)
            term = jnp.where(line < 2 * count, term, jnp.where(line < 2 * count + cols, fence, 0.0))
            extra2[b, h] = term.astype(BF16)

    def scales(temp):
        return [jnp.broadcast_to(temp[:, h:h + 1] * (LOG2E / math.sqrt(size)), (size, LANES)) for h in range(heads)]

    def scaled_t(queries_t, temp):
        factors = [jnp.concatenate([one] * (queries_t.shape[1] // LANES), axis=1) for one in temp]
        return (queries_t * jnp.concatenate(factors, axis=0)).astype(BF16)

    scale_lon = scales(temp_lon)
    norm_all = whole(norm_out.at[pl.ds(0, n_lon - 1)], norm_out.at[pl.ds(0, n_lon - 1)], s1.at[0], r1.at[0])
    norm_all.wait_recv()

    nlon = n_lon * width
    normed = norm_in[...].reshape(nlon, depth)
    keys = mm(normed, wk1[...]).astype(BF16)
    both_t = mm_nt(wqv1[...], normed)
    queries_t = scaled_t(both_t[:depth], scale_lon)
    values_t = both_t[depth:].astype(BF16)
    key_extra = ktab[...].reshape(nlon, LANES)
    pad = jnp.zeros((LANES - 16, LANES), BF16)

    def send_att(slot, peer, group):
        index = slot * n_lon + peer
        return pltpu.make_async_remote_copy(
            src_ref=att_out.at[index], dst_ref=att_in.at[group * rows + me_lon], send_sem=s3.at[0],
            recv_sem=r3.at[group // half], device_id=(peer, lat_at(slot)), device_id_type=MESH,
        )

    units = [(b, h) for b in range(2) for h in range(0, heads, 2)]
    row_work = Attention(
        keys, key_extra, queries_t, lambda b, h: jnp.concatenate([extra1[b, h], pad], axis=0), values_t, size
    )

    def row_done(b, h):
        if h < heads - 2:
            return
        att = row_work.taken(b, heads)
        att_out[b * half * n_lon:(b + 1) * half * n_lon] = att.reshape(half * n_lon, cols, depth).astype(BF16)
        if b == 0:
            pl.semaphore_wait(plane_sem, n_lon - 1)
            for step in range(half):
                slot = step + (1 - side) * (half - 1 - 2 * step)
                for hop in order + [0]:
                    send_att(slot, partner(me_lon, hop, n_lon), own).start()
        else:
            for step in list(range(1, half)) + [0]:
                for hop in order + [0]:
                    if step or hop:
                        slot = half + lax.rem(own + step, half)
                        send_att(slot, partner(me_lon, hop, n_lon), half + own).start()

    staggered(row_work.stages, units, row_done)
    my_slot = (half + own) * rows + me_lon
    att_in[pl.ds(my_slot, 1)] = att_out[pl.ds((half + own) * n_lon + me_lon, 1)]

    for name in ("wo1", "wq2", "wk2", "wv2", "wo2", "wg", "wu", "wd", "gain_lat", "gain_mlp"):
        loads[name].wait()
    wqv2[:depth] = wq2[...].T
    wqv2[depth:] = wv2[...].T
    scale_lat = scales(temp_lat)
    field_all = whole(field_out.at[pl.ds(0, n_lat - 1)], field_in.at[pl.ds(0, n_lat - 1)], s2.at[0], r2.at[0])
    field_all.wait_recv()

    near_all = whole(att_out.at[pl.ds(0, count // 2 - 1)], att_in.at[pl.ds(0, count // 2 - 1)], s3.at[0], r3.at[1])
    far_all = whole(att_out.at[pl.ds(0, count // 2)], att_in.at[pl.ds(0, count // 2)], s3.at[0], r3.at[0])
    att_all = whole(att_out.at[pl.ds(0, total - 1)], att_in.at[pl.ds(0, total - 1)], s3.at[0], r3.at[0])
    near_all.wait_recv()
    far_all.wait_recv()

    resid = field_in[...].astype(F32).reshape(cells, depth)
    attended = att_in[...].astype(F32).reshape(cells, depth).astype(BF16)
    first = resid + mm(attended, wo1[...])
    normed = normalize(first, gain_lat[...])
    keys = mm(normed, wk2[...]).astype(BF16)
    both_t = mm_nt(wqv2[...], normed)
    queries_t = scaled_t(both_t[:depth], scale_lat)
    values_t = both_t[depth:].astype(BF16)
    ff = wg.shape[1]
    step_ff = min(ff, 256)

    def send_upd(slot):
        return pltpu.make_async_remote_copy(
            src_ref=upd_out.at[slot], dst_ref=my_cols(out), send_sem=s4.at[0], recv_sem=r4.at[0],
            device_id=(me_lon, lat_at(slot)), device_id_type=MESH,
        )

    col_work = Attention(keys, onehot[...], queries_t, lambda b, h: extra2[b, h], values_t, size)

    def col_done(b, h):
        if h < heads - 2:
            return
        second = first[b * LANES:(b + 1) * LANES] + mm(col_work.taken(b, heads).astype(BF16), wo2[...])
        normed = normalize(second, gain_mlp[...])
        for f in range(0, ff, step_ff):
            gate = mm(normed, wg[:, f:f + step_ff])
            upper = mm(normed, wu[:, f:f + step_ff])
            hidden = (gate * (0.5 * jnp.tanh(0.5 * gate) + 0.5) * upper).astype(BF16)
            second = second + mm(hidden, wd[f:f + step_ff, :])
        upd_out[b * half:(b + 1) * half] = second.reshape(half, rows, cols, depth).astype(BF16)
        if b == 0:
            new = [send_upd(step + (1 - side) * (half - 1 - 2 * step)) for step in range(half)]
        else:
            new = [send_upd(half + lax.rem(own + step, half)) for step in range(1, half)]
        for copy in new:
            copy.start()

    staggered(col_work.stages, units, col_done)
    mine = pltpu.make_async_copy(upd_out.at[half + own], my_cols(out), s4.at[1])
    mine.start()
    norm_all.wait_send()
    field_all.wait_send()
    att_all.wait_send()
    mine.wait()
    upd_all = whole(upd_out.at[pl.ds(0, n_lat - 1)], upd_out.at[pl.ds(0, n_lat - 1)], s4.at[0], r4.at[0])
    upd_all.wait_send()
    upd_all.wait_recv()


def fused_body(
    fields, norm_lon, query_lon, key_lon, value_lon, out_lon, temp_lon, bias_lon,
    norm_lat, query_lat, key_lat, value_lat, out_lat, temp_lat, bias_lat,
    norm_mlp, w_gate, w_up, w_down,
):
    rows, width, depth = fields.shape
    heads = temp_lon.shape[0]
    n_lon, n_lat = lax.axis_size("lon"), lax.axis_size("lat")
    cols = width // n_lat
    nlon = width * n_lon
    total = n_lon * n_lat
    cells = rows * width
    place = np.arange(nlon).reshape(n_lon, n_lat, cols).transpose(1, 0, 2).reshape(nlon)
    turn = place * (2.0 * math.pi / nlon)
    waves = np.stack([np.cos(turn)] * 4 + [np.sin(turn)] * 4, axis=1).astype(np.float32)
    high = waves.astype(jnp.bfloat16).astype(np.float32)
    ktab = np.zeros((nlon, LANES), np.float32)
    ktab[:, :8] = np.where(np.arange(8)[None] % 4 < 2, high, waves - high)
    ktab = ktab.astype(jnp.bfloat16).reshape(n_lat, n_lon * cols, LANES)
    qtab = np.zeros((2, 16, LANES), np.float32)
    qtab[:, :8] = waves.reshape(2, LANES, 8).transpose(0, 2, 1)
    hbm = pl.BlockSpec(memory_space=pl.ANY)
    weights = (query_lon, key_lon, value_lon, out_lon, query_lat, key_lat, value_lat, out_lat,
               w_gate, w_up, w_down)
    dma = pltpu.SemaphoreType.DMA
    updated = pl.pallas_call(
        functools.partial(block_kernel, n_lon, n_lat, rows, width, depth, heads),
        out_shape=pltpu.VMEM((rows, width, depth), BF16),
        in_specs=[hbm] * 21,
        out_specs=hbm,
        scratch_shapes=[pltpu.VMEM((rows, width, depth), BF16)]
        + [pltpu.VMEM((1, depth), F32)] * 3
        + [pltpu.VMEM((1, heads), F32)] * 4
        + [pltpu.VMEM(ktab.shape, BF16), pltpu.VMEM(qtab.shape, F32)]
        + [pltpu.VMEM(w.shape, w.dtype) for w in weights]
        + [
            pltpu.VMEM((rows, n_lat, cols, depth), BF16),
            pltpu.VMEM((n_lat, n_lon, cols, depth), BF16),
            pltpu.VMEM((n_lat, rows, cols, depth), BF16),
            pltpu.VMEM((n_lat, rows, cols, depth), BF16),
            pltpu.VMEM((total, cols, depth), BF16),
            pltpu.VMEM((n_lat * rows, cols, depth), BF16),
            pltpu.VMEM((n_lat, rows, cols, depth), BF16),
            pltpu.VMEM((2 * depth, depth), BF16),
            pltpu.VMEM((2 * depth, depth), BF16),
            pltpu.VMEM((2, heads, 16, LANES), BF16),
            pltpu.VMEM((2, heads, LANES, LANES), BF16),
            pltpu.VMEM((cells, LANES), BF16),
            dma((24,)),
            dma((1,)), dma((1,)),
            dma((1,)), dma((1,)),
            dma((1,)), dma((2,)),
            dma((2,)), dma((1,)),
            pltpu.SemaphoreType.REGULAR((n_lat,)),
            pltpu.SemaphoreType.REGULAR,
        ],
        compiler_params=pltpu.CompilerParams(collective_id=0, has_side_effects=True),
    )(
        fields, norm_lon[None], norm_lat[None], norm_mlp[None], temp_lon[None], bias_lon[None],
        temp_lat[None], bias_lat[None],
        jnp.asarray(ktab), jnp.asarray(qtab), *weights,
    )
    return updated


def fits(rows, width, n_lon, n_lat, heads, depth):
    return (
        rows == n_lon and n_lat % 2 == 0 and width == 8 * n_lat and rows * width == 2 * LANES
        and width * n_lon == 2 * LANES and 2 * n_lat * rows + width // n_lat <= LANES
        and LANES % (depth // heads) == 0 and LANES // (depth // heads) % 2 == 0
    )


def choose(*args):
    rows, width, _ = args[0].shape
    n_lon, n_lat = lax.axis_size("lon"), lax.axis_size("lat")
    if fits(rows, width, n_lon, n_lat, args[6].shape[0], args[0].shape[2]):
        return fused_body(*args)
    return body(*args)


def solution(mesh):
    in_specs = (P("lat", "lon", None),) + (P(),) * 18
    out_specs = P("lat", "lon", None)
    return jax.shard_map(choose, mesh=mesh, in_specs=in_specs, out_specs=out_specs, check_vma=False)
```

```python
import math

import jax
import jax.numpy as jnp
import functools
import numpy as np
from jax import lax
from jax.experimental import pallas as pl
from jax.experimental.pallas import tpu as pltpu
from jax.sharding import PartitionSpec as P


def normalize(values, gain):
    factor = lax.rsqrt(jnp.mean(values * values, axis=-1, keepdims=True) + 1e-06)
    return (values * factor * gain).astype(jnp.bfloat16)


def project(values, weight):
    return jnp.dot(values, weight, preferred_element_type=jnp.float32).astype(jnp.bfloat16)


def attend_lat(queries, keys, values, temp, bias):
    count, cols, depth = queries.shape
    heads = temp.shape[0]
    size = depth // heads
    qh = queries.reshape(count, cols, heads, size)
    kh = keys.reshape(count, cols, heads, size)
    vh = values.reshape(count, cols, heads, size)
    scores = jnp.einsum("ichd,jchd->chij", qh, kh, preferred_element_type=jnp.float32)
    place = jnp.arange(count, dtype=jnp.int32)
    spread = jnp.abs(place[:, None] - place[None, :]).astype(jnp.float32) / count
    scores = (
        scores * (temp / math.sqrt(size))[None, :, None, None]
        + bias[None, :, None, None] * spread[None, None]
    )
    expo = jnp.exp(scores - jnp.max(scores, axis=-1, keepdims=True))
    denom = jnp.sum(expo, axis=-1)
    mixed = jnp.einsum(
        "chij,jchd->ichd", expo.astype(jnp.bfloat16), vh, preferred_element_type=jnp.float32
    )
    mixed = mixed / jnp.transpose(denom, (2, 0, 1))[..., None]
    return mixed.astype(jnp.bfloat16).reshape(count, cols, depth)


def body(
    fields,
    norm_lon,
    query_lon,
    key_lon,
    value_lon,
    out_lon,
    temp_lon,
    bias_lon,
    norm_lat,
    query_lat,
    key_lat,
    value_lat,
    out_lat,
    temp_lat,
    bias_lat,
    norm_mlp,
    w_gate,
    w_up,
    w_down,
):
    rows, width, depth = fields.shape
    heads = temp_lon.shape[0]
    size = depth // heads
    total_lon = width * lax.axis_size("lon")
    resid = fields.astype(jnp.float32)
    normed = normalize(resid, norm_lon)
    scale_lon = temp_lon / math.sqrt(size)
    query_place = lax.axis_index("lon") * width + jnp.arange(width, dtype=jnp.int32)
    queries = project(normed, query_lon).reshape(rows, width, heads, size)
    piece = lax.all_gather(normed, "lon", axis=1, tiled=True)
    keys = project(piece, key_lon)
    count = keys.shape[1]
    key_place = jnp.arange(count, dtype=jnp.int32)
    angle = (query_place[:, None] - key_place[None, :]).astype(jnp.float32) * (
        2.0 * math.pi / total_lon
    )
    wave = jnp.cos(angle)

    def one_row(items):
        query_row, key_row, value_row, peak, total, accum = items
        key_heads = key_row.reshape(count, heads, size)
        value_heads = value_row.reshape(count, heads, size)
        scores = jnp.einsum(
            "ihd,jhd->hij", query_row, key_heads, preferred_element_type=jnp.float32
        )
        scores = scores * scale_lon[:, None, None] + bias_lon[:, None, None] * wave[None]
        fresh = jnp.maximum(peak, jnp.max(scores, axis=-1))
        shrink = jnp.exp(peak - fresh)
        expo = jnp.exp(scores - fresh[..., None])
        total = total * shrink + jnp.sum(expo, axis=-1)
        mixed = jnp.einsum(
            "hij,jhd->ihd",
            expo.astype(jnp.bfloat16),
            value_heads,
            preferred_element_type=jnp.float32,
        )
        accum = accum.reshape(width, heads, size) * jnp.transpose(shrink)[:, :, None] + mixed
        return (fresh, total, accum.reshape(width, depth))

    peak = jnp.full((rows, heads, width), -1e30, jnp.float32)
    total = jnp.zeros((rows, heads, width), jnp.float32)
    accum = jnp.zeros((rows, width, depth), jnp.float32)
    peak, total, accum = lax.map(
        one_row, (queries, keys, project(piece, value_lon), peak, total, accum)
    )
    attended = accum.reshape(rows, width, heads, size) / jnp.transpose(total, (0, 2, 1))[..., None]
    attended = attended.astype(jnp.bfloat16).reshape(rows, width, depth)
    first = resid + jnp.dot(attended, out_lon, preferred_element_type=jnp.float32)
    normed_lat = normalize(first, norm_lat)
    query_col = project(normed_lat, query_lat)
    key_col = project(normed_lat, key_lat)
    value_col = project(normed_lat, value_lat)
    query_col, key_col, value_col = (
        lax.all_to_all(query_col, "lat", split_axis=1, concat_axis=0, tiled=True),
        lax.all_to_all(key_col, "lat", split_axis=1, concat_axis=0, tiled=True),
        lax.all_to_all(value_col, "lat", split_axis=1, concat_axis=0, tiled=True),
    )
    mixed_lat = attend_lat(query_col, key_col, value_col, temp_lat, bias_lat)
    returned = lax.all_to_all(mixed_lat, "lat", split_axis=0, concat_axis=1, tiled=True)
    second = first + jnp.dot(returned, out_lat, preferred_element_type=jnp.float32)
    normed_mlp = normalize(second, norm_mlp)
    gate = jnp.dot(normed_mlp, w_gate, preferred_element_type=jnp.float32)
    upper = jnp.dot(normed_mlp, w_up, preferred_element_type=jnp.float32)
    hidden = (jax.nn.silu(gate) * upper).astype(jnp.bfloat16)
    return (second + jnp.dot(hidden, w_down, preferred_element_type=jnp.float32)).astype(
        jnp.bfloat16
    )


NT = (((1,), (1,)), ((), ()))
MESH = pl.DeviceIdType.MESH
F32 = jnp.float32
BF16 = jnp.bfloat16
LANES = 128
LOG2E = math.log2(math.e)


def mm(a, b):
    return jnp.dot(a, b, preferred_element_type=F32)


def mm_nt(a, b):
    return lax.dot_general(a, b, NT, preferred_element_type=F32)


def iota(shape, dim):
    return lax.broadcasted_iota(jnp.int32, shape, dim)


def partner(me, step, n):
    if n & (n - 1):
        return lax.rem(me + step, n)
    bits = [b for b in range(n.bit_length()) if step >> b & 1]
    return sum((1 - 2 * lax.rem(me // (1 << b), 2)) * (1 << b) for b in bits) + me


def far_first(n):
    return sorted(range(1, n), key=lambda step: -(2 * (step >> 1).bit_count() + (step & 1)))


def split_pairs(values, odd):
    high = values.astype(BF16).astype(F32)
    return jnp.where(odd, values - high, high)


class Quads:
    def __init__(self, left, right, table, values, size):
        self.left, self.right, self.table, self.values, self.size = left, right, table, values, size
        self.stages = (self.scores, self.weights, self.mixed, self.turned)
        self.held = {}

    def scores(self, *unit):
        scores = mm(self.left(*unit), self.right(*unit))
        if self.table is not None:
            scores = scores + self.table(*unit)
        self.held[unit] = scores

    def weights(self, *unit):
        scores = self.held[unit]
        self.held[unit] = jnp.exp2((scores - jnp.max(scores, axis=0, keepdims=True)).astype(BF16))

    def mixed(self, *unit):
        self.held[unit] = mm(self.values(*unit), self.held[unit])

    def turned(self, *unit):
        mixed = self.held[unit]
        share = 1.0 / mixed[LANES:LANES + 1, :]
        parts = []
        for i in range(LANES // self.size):
            lane = slice(i // 2 * LANES, (i // 2 + 1) * LANES)
            parts.append(mixed[i * self.size:(i + 1) * self.size, lane] * share[:, lane])
        both = jnp.concatenate(parts, axis=0).T
        odd = lax.rem(iota((LANES // 2, LANES), 1) // self.size, 2) == 1
        self.held[unit] = jnp.where(odd, both[LANES // 2:], both[:LANES // 2])


class Pairs(Quads):
    def turned(self, b, h):
        mixed = self.held[b, h]
        share = 1.0 / mixed[2 * self.size:2 * self.size + 1, :]
        self.held[b, h] = jnp.concatenate(
            [mixed[:self.size, :LANES] * share[:, :LANES], mixed[self.size:2 * self.size, LANES:] * share[:, LANES:]],
            axis=0,
        )
        if h % 4 == 2:
            self.held[b, h] = jnp.concatenate([self.held.pop((b, h - 2)), self.held[b, h]], axis=0).T


def pair_of(queries_t, h, size):
    group = h // (LANES // size)
    blank = jnp.zeros((size, LANES), BF16)
    pieces = []
    for g in range(group * (LANES // size), (group + 1) * (LANES // size)):
        rows = queries_t[g * size:(g + 1) * size]
        pieces.append(jnp.concatenate([rows if g == h else blank, rows if g == h + 1 else blank], axis=1))
    return jnp.concatenate(pieces, axis=0)


def side_by_side(natural, turned, parity, group, size):
    lanes = iota((size, LANES), 1)
    keep = [(lanes < LANES // 2).astype(F32).astype(BF16), (lanes >= LANES // 2).astype(F32).astype(BF16)]
    blank = jnp.zeros((size, LANES), BF16)
    pieces = []
    for i in range(LANES // size):
        h = group * (LANES // size) + i
        rows = (natural if i % 2 == parity else turned)[h * size:(h + 1) * size] * keep[i % 2]
        pieces.append(jnp.concatenate([rows, blank] if i < 2 else [blank, rows], axis=1))
    return jnp.concatenate(pieces, axis=0)


def per_head(values, group, shape):
    lanes = iota(shape, 1) // (LANES // 2)
    out = jnp.broadcast_to(values[:, 4 * group:4 * group + 1], shape)
    for i in range(1, 4):
        out = jnp.where(lanes == i, values[:, 4 * group + i:4 * group + i + 1], out)
    return out


def root_mean(values):
    return lax.rsqrt(jnp.mean(values * values, axis=-1, keepdims=True) + 1e-06)


def halves_turned(rows):
    half = LANES // 2
    return jnp.concatenate([rows[(i ^ 1) * half:((i ^ 1) + 1) * half] for i in range(rows.shape[0] // half)], axis=0)


def staggered(stages, units, after):
    for step in range(len(units) + len(stages) - 1):
        for s, stage in enumerate(stages):
            if 0 <= step - s < len(units):
                stage(*units[step - s])
        if step >= len(stages) - 1:
            after(*units[step - len(stages) + 1])


def block_kernel(
    n_lon, n_lat, rows, width, depth, heads,
    fields_h, gain_lon_h, gain_lat_h, gain_mlp_h, temp_lon_h, bias_lon_h, temp_lat_h, bias_lat_h,
    ktab_h, qtab_h, wq1_h, wk1_h, wv1_h, wo1_h, wq2_h, wk2_h, wv2_h, wo2_h, wg_h, wu_h, wd_h,
    out,
    fields, gain_lon, gain_lat, gain_mlp, temp_lon, bias_lon, temp_lat, bias_lat,
    ktab, qtab, wq1, wk1, wv1, wo1, wq2, wk2, wv2, wo2, wg, wu, wd,
    norm_out, norm_in, field_out, field_in, att_out, att_in, upd_out,
    wqv1, wqv2, extra1, tables, resid, shuffle, hidden,
    local_sem, s1, r1, s2, r2, s3, r3, s4, r4, line_sem, plane_sem,
):
    me_lon = lax.axis_index("lon")
    me_lat = lax.axis_index("lat")
    total = n_lon * n_lat
    size = depth // heads
    cols = width // n_lat
    count = n_lat * rows
    cells = rows * width
    half = n_lat // 2
    block = half * rows
    side = me_lat // half
    own = lax.rem(me_lat, half)

    def lat_at(slot):
        if slot < half:
            return side * slot + (1 - side) * (n_lat - 1 - slot)
        return side * half + lax.rem(own + 1 + slot - half, half)

    def slot_of(lat, viewer):
        upper, seen = lat // half, viewer // half
        distant = upper + seen - 2 * upper * seen
        far_slot = upper * (n_lat - 1 - lat) + (1 - upper) * lat
        near_slot = half + lax.rem(lat + 2 * half - 1 - viewer + 2 * half * n_lat, half)
        return distant * far_slot + (1 - distant) * near_slot

    loads = {}

    def load(name, src, dst):
        loads[name] = pltpu.make_async_copy(src, dst, local_sem.at[len(loads)])
        loads[name].start()

    load("fields", fields_h, fields)
    load("gain_lon", gain_lon_h, gain_lon)
    barrier = pltpu.get_barrier_semaphore()
    order = far_first(n_lon)

    def signal_plane(sem):
        for step in order:
            pl.semaphore_signal(
                sem, inc=1, device_id=(partner(me_lon, step, n_lon), me_lat), device_id_type=MESH
            )

    def signal_line(sem):
        @pl.when(me_lat > 0)
        def _():
            pl.semaphore_signal(sem, inc=1, device_id=(me_lon, me_lat - 1), device_id_type=MESH)

        @pl.when(me_lat < n_lat - 1)
        def _():
            pl.semaphore_signal(sem, inc=1, device_id=(me_lon, me_lat + 1), device_id_type=MESH)

    beside = jnp.minimum(me_lat, 1) + jnp.minimum(n_lat - 1 - me_lat, 1)
    signal_plane(barrier)
    signal_line(barrier)
    for slot in range(n_lat):
        load(f"ktab{slot}", ktab_h.at[lat_at(slot)], ktab.at[slot])
        load(f"qtab{slot}", qtab_h.at[lat_at(slot)], qtab.at[slot])
    for name, src, dst in [
        ("wq1", wq1_h, wq1), ("wk1", wk1_h, wk1), ("wv1", wv1_h, wv1), ("temp_lon", temp_lon_h, temp_lon),
        ("bias_lon", bias_lon_h, bias_lon), ("temp_lat", temp_lat_h, temp_lat), ("bias_lat", bias_lat_h, bias_lat),
        ("wo1", wo1_h, wo1), ("wq2", wq2_h, wq2), ("wk2", wk2_h, wk2), ("wv2", wv2_h, wv2), ("wo2", wo2_h, wo2),
        ("wg", wg_h, wg), ("wu", wu_h, wu), ("wd", wd_h, wd), ("gain_lat", gain_lat_h, gain_lat),
        ("gain_mlp", gain_mlp_h, gain_mlp),
    ]:
        load(name, src, dst)

    loads["fields"].wait()
    loads["gain_lon"].wait()
    wide = fields[...].astype(F32)
    factor = lax.rsqrt(jnp.mean(wide * wide, axis=-1, keepdims=True) + 1e-06)
    scaled = (wide * factor * gain_lon[...][None]).reshape(rows, n_lat, cols, depth).astype(BF16)
    pieces = wide.reshape(rows, n_lat, cols, depth).astype(BF16)
    for a in range(n_lat):
        norm_out[:, pl.ds(slot_of(a, me_lat), 1)] = scaled[:, a:a + 1]
        field_out[a] = pieces[:, a]

    pl.semaphore_wait(barrier, n_lon - 1 + beside)

    def my_cols(ref):
        return ref.at[:, pl.ds(pl.multiple_of(me_lat * cols, cols), cols), :]

    def send_norm(step):
        peer = partner(me_lon, step, n_lon)
        return pltpu.make_async_remote_copy(
            src_ref=norm_out.at[peer], dst_ref=norm_in.at[:, me_lon],
            send_sem=s1.at[0], recv_sem=r1.at[0], device_id=(peer, me_lat), device_id_type=MESH,
        )

    def send_field(peer):
        slot = slot_of(me_lat, peer)
        return pltpu.make_async_remote_copy(
            src_ref=field_out.at[peer], dst_ref=field_in.at[slot], send_sem=s2.at[0],
            recv_sem=r2.at[0], device_id=(me_lon, peer), device_id_type=MESH,
        )

    def send_fields(hop):
        @pl.when(me_lat >= hop)
        def _():
            send_field(me_lat - hop).start()

        @pl.when(me_lat + hop < n_lat)
        def _():
            send_field(me_lat + hop).start()

    def whole(src, dst, sends, recvs):
        return pltpu.make_async_remote_copy(
            src_ref=src, dst_ref=dst, send_sem=sends, recv_sem=recvs,
            device_id=(me_lon, me_lat), device_id_type=MESH,
        )

    for step in order:
        send_norm(step).start()
    for hop in range(1, n_lat):
        if hop > 1:
            pl.semaphore_wait(line_sem.at[hop - 1], beside)
        if hop < n_lat - 1:
            signal_line(line_sem.at[hop])
        send_fields(hop)
    signal_plane(plane_sem)
    norm_in[:, pl.ds(me_lon, 1)] = norm_out[pl.ds(me_lon, 1)].reshape(n_lat, 1, cols, depth)
    field_in[n_lat - 1:] = field_out[pl.ds(me_lat, 1)]

    for name in ["wq1", "wk1", "wv1", "temp_lon", "bias_lon", "temp_lat", "bias_lat"] + [
        f"{kind}{slot}" for slot in range(n_lat) for kind in ("ktab", "qtab")
    ]:
        loads[name].wait()
    wqv1[:depth] = wq1[...].T
    wqv1[depth:] = wv1[...].T
    groups = depth // LANES
    shape = (16, 2 * LANES)
    odd = lax.rem(iota(shape, 0), 2) == 1
    halves = iota((16, LANES), 1) < LANES // 2
    for b in range(2):
        wave = jnp.where(halves, qtab[2 * b], qtab[2 * b + 1])
        wave = jnp.concatenate([wave, wave], axis=1)
        for h in range(0, heads, 2):
            weight = jnp.where(
                iota(shape, 1) < LANES, bias_lon[:, h:h + 1], bias_lon[:, h + 1:h + 2]
            ) * LOG2E
            extra1[b, h // 2] = split_pairs(weight * wave, odd).astype(BF16)
    hold = half * rows
    shape = (LANES, 2 * LANES)
    key_cell, query_cell = iota(shape, 0), lax.rem(iota(shape, 1), LANES // 2)

    def lat_value(spot, distant):
        group = spot // rows
        value = jnp.zeros(shape, jnp.int32)
        for g in range(half):
            value = jnp.where(group == g, lat_at(g if distant else half + g), value)
        return value * rows + lax.rem(spot, rows)

    key_far, key_near = lat_value(lax.rem(key_cell, hold), True), lat_value(lax.rem(key_cell, hold), False)
    same = lax.rem(key_cell, LANES // 2) // hold == query_cell // hold
    for g in range(groups):
        weight = per_head(bias_lat, g, shape) * (LOG2E / count)
        for f in range(2):
            there = lat_value(lax.rem(query_cell, hold), f == 0)
            for c in range(2):
                first_part = key_cell < LANES // 2
                here = jnp.where(first_part, key_far, key_near) if c == 0 else jnp.where(first_part, key_near, key_far)
                tables[f, c, g] = jnp.where(same, weight * jnp.abs(here - there).astype(F32), -1e30)

    def scales(temp):
        return [jnp.broadcast_to(temp[:, h:h + 1] * (LOG2E / math.sqrt(size)), (size, LANES)) for h in range(heads)]

    def scaled_t(queries_t, temp):
        factors = [jnp.concatenate([one] * (queries_t.shape[1] // LANES), axis=1) for one in temp]
        return (queries_t * jnp.concatenate(factors, axis=0)).astype(BF16)

    scale_lon = scales(temp_lon)
    norm_all = whole(norm_out.at[pl.ds(0, n_lon - 1)], norm_out.at[pl.ds(0, n_lon - 1)], s1.at[0], r1.at[0])
    norm_all.wait_recv()

    nlon = n_lon * width
    normed = norm_in[...].reshape(nlon, depth)
    keys = mm(normed, wk1[...]).astype(BF16)
    both_t = mm_nt(wqv1[...], normed)
    queries_t = scaled_t(both_t[:depth], scale_lon)
    values_t = both_t[depth:].astype(BF16)
    key_extra = ktab[...].reshape(nlon, LANES)[:, :16]
    ones = jnp.ones((16, nlon), BF16)

    row_work = Pairs(
        lambda b, h: jnp.concatenate([keys[:, h // 4 * LANES:(h // 4 + 1) * LANES], key_extra], axis=1),
        lambda b, h: jnp.concatenate(
            [pair_of(queries_t[:, b * LANES:(b + 1) * LANES], h, size), extra1[b, h // 2]], axis=0
        ),
        None,
        lambda b, h: jnp.concatenate([values_t[h * size:(h + 2) * size], ones], axis=0),
        size,
    )

    distant_slot = slot_of(me_lat, (1 - side) * half)

    def send_att(slot, peer):
        group = distant_slot if slot < half else half + (n_lat - 2 - slot) % half
        return pltpu.make_async_remote_copy(
            src_ref=att_out.at[slot * n_lon + peer], dst_ref=att_in.at[group * rows + me_lon], send_sem=s3.at[0],
            recv_sem=r3.at[min(slot // half, 1)], device_id=(peer, lat_at(slot)), device_id_type=MESH,
        )

    def row_done(b, h):
        if h < heads - 2:
            return
        att = jnp.concatenate([row_work.held.pop((b, k)) for k in range(2, heads, 4)], axis=1)
        att_out[b * half * n_lon:(b + 1) * half * n_lon] = att.reshape(half * n_lon, cols, depth).astype(BF16)
        if b == 0:
            pl.semaphore_wait(plane_sem, n_lon - 1)
        for hop in order + [0]:
            for slot in range(b * half, (b + 1) * half):
                if hop or slot < n_lat - 1:
                    send_att(slot, partner(me_lon, hop, n_lon)).start()

    staggered(row_work.stages, [(b, h) for b in range(2) for h in range(0, heads, 2)], row_done)
    att_in[pl.ds((n_lat - 1) * rows + me_lon, 1)] = att_out[pl.ds((n_lat - 1) * n_lon + me_lon, 1)]

    for name in ("wo1", "wq2", "wk2", "wv2", "wo2", "wg", "wu", "wd", "gain_lat", "gain_mlp"):
        loads[name].wait()
    wqv2[:depth] = wq2[...].T
    wqv2[depth:] = wv2[...].T
    scale_lat = scales(temp_lat)
    field_all = whole(field_out.at[pl.ds(0, n_lat - 1)], field_in.at[pl.ds(0, n_lat - 1)], s2.at[0], r2.at[0])
    field_all.wait_recv()

    near_all = whole(att_out.at[pl.ds(0, count // 2 - 1)], att_in.at[pl.ds(0, count // 2 - 1)], s3.at[0], r3.at[1])
    far_all = whole(att_out.at[pl.ds(0, count // 2)], att_in.at[pl.ds(0, count // 2)], s3.at[0], r3.at[0])
    att_all = whole(att_out.at[pl.ds(0, total - 1)], att_in.at[pl.ds(0, total - 1)], s3.at[0], r3.at[0])
    starts = [list(range(cols)), list(range(cols // 2, cols)) + list(range(cols // 2))]

    def by_column(f, values):
        values = values.astype(F32).reshape(LANES, depth)
        parts = []
        for g in range(groups):
            shuffle[groups * f + g] = values[:, g * LANES:(g + 1) * LANES]
            parts.append([shuffle[groups * f + g, pl.ds(c, block, stride=cols), :] for c in starts[f]])
        return jnp.concatenate([jnp.concatenate(part, axis=0) for part in parts], axis=1)

    for f in range(2):
        resid[f * LANES:(f + 1) * LANES] = by_column(f, field_in[f * half:(f + 1) * half])

    firsts, keys2, queries2, turned2, values2 = {}, {}, {}, {}, {}

    def project_columns(f):
        attended = by_column(f, att_in[f * block:(f + 1) * block]).astype(BF16)
        firsts[f] = resid[f * LANES:(f + 1) * LANES] + mm(attended, wo1[...])
        gained = (firsts[f] * gain_lat[...]).astype(BF16)
        factor = root_mean(firsts[f])
        across = jnp.broadcast_to(factor, (LANES, LANES)).T[:1]
        turned = jnp.broadcast_to(halves_turned(factor), (LANES, LANES)).T[:1]
        keys2[f] = (mm(gained, wk2[...]) * factor).astype(BF16)
        both_t = mm_nt(wqv2[...], gained)
        queries2[f] = scaled_t(both_t[:depth], [one * across for one in scale_lat])
        turned2[f] = scaled_t(mm_nt(wqv2[:depth], halves_turned(gained)), [one * turned for one in scale_lat])
        values2[f] = (both_t[depth:] * across).astype(BF16)

    near_all.wait_recv()
    project_columns(1)
    far_all.wait_recv()
    project_columns(0)
    part = LANES // 2
    low = (iota((LANES, LANES), 1) < part).astype(F32).astype(BF16)
    high = (iota((LANES, LANES), 1) >= part).astype(F32).astype(BF16)
    ones = jnp.ones((16, LANES), BF16)

    def column_keys(f, c, g):
        lane = slice(g * LANES, (g + 1) * LANES)
        return jnp.concatenate([keys2[c][:part, lane], keys2[1 - c][part:, lane]], axis=0)

    def column_values(f, c, g):
        row = slice(g * LANES, (g + 1) * LANES)
        return jnp.concatenate([values2[c][row] * low + values2[1 - c][row] * high, ones], axis=0)

    col_work = Quads(
        column_keys,
        lambda f, c, g: side_by_side(queries2[f], turned2[f], c if f == 0 else 1 - c, g, size),
        lambda f, c, g: tables[f, c, g],
        column_values,
        size,
    )
    ff = wg.shape[1]
    step_ff = min(ff, 256)

    def send_upd(slot):
        return pltpu.make_async_remote_copy(
            src_ref=upd_out.at[slot], dst_ref=my_cols(out), send_sem=s4.at[0], recv_sem=r4.at[0],
            device_id=(me_lon, lat_at(slot)), device_id_type=MESH,
        )

    def col_done(f, c, g):
        if c != (1 if f == 0 else 0) or g < groups - 1:
            return
        att = jnp.concatenate(
            [jnp.concatenate([col_work.held.pop((f, k, g)) for g in range(groups)], axis=1)
             for k in ((0, 1) if f == 0 else (1, 0))], axis=0
        )
        second = firsts[f] + mm(att.astype(BF16), wo2[...])
        gained = (second * gain_mlp[...]).astype(BF16)
        factor = root_mean(second)
        for k in range(0, ff, step_ff):
            gate = mm(gained, wg[:, k:k + step_ff]) * factor
            upper = mm(gained, wu[:, k:k + step_ff]) * factor
            hidden[:, k:k + step_ff] = (gate * (0.5 * jnp.tanh(0.5 * gate) + 0.5) * upper).astype(BF16)
        second = second + mm(hidden[...], wd[...])
        for i, c in enumerate(starts[f]):
            for g in range(groups):
                shuffle[groups * f + g, pl.ds(c, block, stride=cols), :] = (
                    second[i * block:(i + 1) * block, g * LANES:(g + 1) * LANES]
                )
        updated = jnp.concatenate([shuffle[groups * f + g] for g in range(groups)], axis=1)
        upd_out[f * half:(f + 1) * half] = updated.reshape(half, rows, cols, depth).astype(BF16)
        for slot in range(f * half, (f + 1) * half):
            if slot < n_lat - 1:
                send_upd(slot).start()

    for f in range(2):
        staggered(
            col_work.stages, [(f, c, g) for c in ((0, 1) if f == 0 else (1, 0)) for g in range(groups)], col_done
        )
    mine = pltpu.make_async_copy(upd_out.at[n_lat - 1], my_cols(out), s4.at[1])
    mine.start()
    norm_all.wait_send()
    field_all.wait_send()
    att_all.wait_send()
    mine.wait()
    upd_all = whole(upd_out.at[pl.ds(0, n_lat - 1)], upd_out.at[pl.ds(0, n_lat - 1)], s4.at[0], r4.at[0])
    upd_all.wait_send()
    upd_all.wait_recv()


def fused_body(
    fields, norm_lon, query_lon, key_lon, value_lon, out_lon, temp_lon, bias_lon,
    norm_lat, query_lat, key_lat, value_lat, out_lat, temp_lat, bias_lat,
    norm_mlp, w_gate, w_up, w_down,
):
    rows, width, depth = fields.shape
    heads = temp_lon.shape[0]
    n_lon, n_lat = lax.axis_size("lon"), lax.axis_size("lat")
    cols = width // n_lat
    nlon = width * n_lon
    total = n_lon * n_lat
    cells = rows * width
    place = np.arange(nlon).reshape(n_lon, n_lat, cols).transpose(1, 0, 2).reshape(nlon)
    turn = place * (2.0 * math.pi / nlon)
    waves = np.stack([np.cos(turn)] * 4 + [np.sin(turn)] * 4, axis=1).astype(np.float32)
    high = waves.astype(jnp.bfloat16).astype(np.float32)
    ktab = np.zeros((nlon, LANES), np.float32)
    ktab[:, :8] = np.where(np.arange(8)[None] % 4 < 2, high, waves - high)
    ktab = ktab.astype(jnp.bfloat16).reshape(n_lat, n_lon * cols, LANES)
    qtab = np.zeros((n_lat, 16, LANES), np.float32)
    qtab[:, :8] = np.tile(waves.reshape(n_lat, LANES // 2, 8).transpose(0, 2, 1), (1, 1, 2))
    hbm = pl.BlockSpec(memory_space=pl.ANY)
    weights = (query_lon, key_lon, value_lon, out_lon, query_lat, key_lat, value_lat, out_lat,
               w_gate, w_up, w_down)
    dma = pltpu.SemaphoreType.DMA
    updated = pl.pallas_call(
        functools.partial(block_kernel, n_lon, n_lat, rows, width, depth, heads),
        out_shape=pltpu.VMEM((rows, width, depth), BF16),
        in_specs=[hbm] * 21,
        out_specs=hbm,
        scratch_shapes=[pltpu.VMEM((rows, width, depth), BF16)]
        + [pltpu.VMEM((1, depth), F32)] * 3
        + [pltpu.VMEM((1, heads), F32)] * 4
        + [pltpu.VMEM(ktab.shape, BF16), pltpu.VMEM(qtab.shape, F32)]
        + [pltpu.VMEM(w.shape, w.dtype) for w in weights]
        + [
            pltpu.VMEM((rows, n_lat, cols, depth), BF16),
            pltpu.VMEM((n_lat, n_lon, cols, depth), BF16),
            pltpu.VMEM((n_lat, rows, cols, depth), BF16),
            pltpu.VMEM((n_lat, rows, cols, depth), BF16),
            pltpu.VMEM((total, cols, depth), BF16),
            pltpu.VMEM((n_lat * rows, cols, depth), BF16),
            pltpu.VMEM((n_lat, rows, cols, depth), BF16),
            pltpu.VMEM((2 * depth, depth), BF16),
            pltpu.VMEM((2 * depth, depth), BF16),
            pltpu.VMEM((2, heads // 2, 16, 2 * LANES), BF16),
            pltpu.VMEM((2, 2, depth // LANES, LANES, 2 * LANES), F32),
            pltpu.VMEM((cells, depth), F32),
            pltpu.VMEM((2 * depth // LANES, LANES, LANES), F32),
            pltpu.VMEM((LANES, w_gate.shape[1]), BF16),
            dma((32,)),
            dma((1,)), dma((1,)),
            dma((1,)), dma((1,)),
            dma((1,)), dma((2,)),
            dma((2,)), dma((1,)),
            pltpu.SemaphoreType.REGULAR((n_lat,)),
            pltpu.SemaphoreType.REGULAR,
        ],
        compiler_params=pltpu.CompilerParams(collective_id=0, has_side_effects=True),
    )(
        fields, norm_lon[None], norm_lat[None], norm_mlp[None], temp_lon[None], bias_lon[None],
        temp_lat[None], bias_lat[None],
        jnp.asarray(ktab), jnp.asarray(qtab), *weights,
    )
    return updated


def fits(rows, width, n_lon, n_lat, heads, depth):
    return (
        rows == n_lon and n_lat % 2 == 0 and width == 8 * n_lat and rows * width == 2 * LANES
        and width * n_lon == 2 * LANES and n_lat == 4 and depth % LANES == 0 and heads * LANES == 4 * depth
    )


def choose(*args):
    rows, width, _ = args[0].shape
    n_lon, n_lat = lax.axis_size("lon"), lax.axis_size("lat")
    if fits(rows, width, n_lon, n_lat, args[6].shape[0], args[0].shape[2]):
        return fused_body(*args)
    return body(*args)


def solution(mesh):
    in_specs = (P("lat", "lon", None),) + (P(),) * 18
    out_specs = P("lat", "lon", None)
    return jax.shard_map(choose, mesh=mesh, in_specs=in_specs, out_specs=out_specs, check_vma=False)
```

```python
import math

import jax
import jax.numpy as jnp
import functools
import numpy as np
from jax import lax
from jax.experimental import pallas as pl
from jax.experimental.pallas import tpu as pltpu
from jax.sharding import PartitionSpec as P


def normalize(values, gain):
    factor = lax.rsqrt(jnp.mean(values * values, axis=-1, keepdims=True) + 1e-06)
    return (values * factor * gain).astype(jnp.bfloat16)


def project(values, weight):
    return jnp.dot(values, weight, preferred_element_type=jnp.float32).astype(jnp.bfloat16)


def attend_lat(queries, keys, values, temp, bias):
    count, cols, depth = queries.shape
    heads = temp.shape[0]
    size = depth // heads
    qh = queries.reshape(count, cols, heads, size)
    kh = keys.reshape(count, cols, heads, size)
    vh = values.reshape(count, cols, heads, size)
    scores = jnp.einsum("ichd,jchd->chij", qh, kh, preferred_element_type=jnp.float32)
    place = jnp.arange(count, dtype=jnp.int32)
    spread = jnp.abs(place[:, None] - place[None, :]).astype(jnp.float32) / count
    scores = (
        scores * (temp / math.sqrt(size))[None, :, None, None]
        + bias[None, :, None, None] * spread[None, None]
    )
    expo = jnp.exp(scores - jnp.max(scores, axis=-1, keepdims=True))
    denom = jnp.sum(expo, axis=-1)
    mixed = jnp.einsum(
        "chij,jchd->ichd", expo.astype(jnp.bfloat16), vh, preferred_element_type=jnp.float32
    )
    mixed = mixed / jnp.transpose(denom, (2, 0, 1))[..., None]
    return mixed.astype(jnp.bfloat16).reshape(count, cols, depth)


def body(
    fields,
    norm_lon,
    query_lon,
    key_lon,
    value_lon,
    out_lon,
    temp_lon,
    bias_lon,
    norm_lat,
    query_lat,
    key_lat,
    value_lat,
    out_lat,
    temp_lat,
    bias_lat,
    norm_mlp,
    w_gate,
    w_up,
    w_down,
):
    rows, width, depth = fields.shape
    heads = temp_lon.shape[0]
    size = depth // heads
    total_lon = width * lax.axis_size("lon")
    resid = fields.astype(jnp.float32)
    normed = normalize(resid, norm_lon)
    scale_lon = temp_lon / math.sqrt(size)
    query_place = lax.axis_index("lon") * width + jnp.arange(width, dtype=jnp.int32)
    queries = project(normed, query_lon).reshape(rows, width, heads, size)
    piece = lax.all_gather(normed, "lon", axis=1, tiled=True)
    keys = project(piece, key_lon)
    count = keys.shape[1]
    key_place = jnp.arange(count, dtype=jnp.int32)
    angle = (query_place[:, None] - key_place[None, :]).astype(jnp.float32) * (
        2.0 * math.pi / total_lon
    )
    wave = jnp.cos(angle)

    def one_row(items):
        query_row, key_row, value_row, peak, total, accum = items
        key_heads = key_row.reshape(count, heads, size)
        value_heads = value_row.reshape(count, heads, size)
        scores = jnp.einsum(
            "ihd,jhd->hij", query_row, key_heads, preferred_element_type=jnp.float32
        )
        scores = scores * scale_lon[:, None, None] + bias_lon[:, None, None] * wave[None]
        fresh = jnp.maximum(peak, jnp.max(scores, axis=-1))
        shrink = jnp.exp(peak - fresh)
        expo = jnp.exp(scores - fresh[..., None])
        total = total * shrink + jnp.sum(expo, axis=-1)
        mixed = jnp.einsum(
            "hij,jhd->ihd",
            expo.astype(jnp.bfloat16),
            value_heads,
            preferred_element_type=jnp.float32,
        )
        accum = accum.reshape(width, heads, size) * jnp.transpose(shrink)[:, :, None] + mixed
        return (fresh, total, accum.reshape(width, depth))

    peak = jnp.full((rows, heads, width), -1e30, jnp.float32)
    total = jnp.zeros((rows, heads, width), jnp.float32)
    accum = jnp.zeros((rows, width, depth), jnp.float32)
    peak, total, accum = lax.map(
        one_row, (queries, keys, project(piece, value_lon), peak, total, accum)
    )
    attended = accum.reshape(rows, width, heads, size) / jnp.transpose(total, (0, 2, 1))[..., None]
    attended = attended.astype(jnp.bfloat16).reshape(rows, width, depth)
    first = resid + jnp.dot(attended, out_lon, preferred_element_type=jnp.float32)
    normed_lat = normalize(first, norm_lat)
    query_col = project(normed_lat, query_lat)
    key_col = project(normed_lat, key_lat)
    value_col = project(normed_lat, value_lat)
    query_col, key_col, value_col = (
        lax.all_to_all(query_col, "lat", split_axis=1, concat_axis=0, tiled=True),
        lax.all_to_all(key_col, "lat", split_axis=1, concat_axis=0, tiled=True),
        lax.all_to_all(value_col, "lat", split_axis=1, concat_axis=0, tiled=True),
    )
    mixed_lat = attend_lat(query_col, key_col, value_col, temp_lat, bias_lat)
    returned = lax.all_to_all(mixed_lat, "lat", split_axis=0, concat_axis=1, tiled=True)
    second = first + jnp.dot(returned, out_lat, preferred_element_type=jnp.float32)
    normed_mlp = normalize(second, norm_mlp)
    gate = jnp.dot(normed_mlp, w_gate, preferred_element_type=jnp.float32)
    upper = jnp.dot(normed_mlp, w_up, preferred_element_type=jnp.float32)
    hidden = (jax.nn.silu(gate) * upper).astype(jnp.bfloat16)
    return (second + jnp.dot(hidden, w_down, preferred_element_type=jnp.float32)).astype(
        jnp.bfloat16
    )


NT = (((1,), (1,)), ((), ()))
MESH = pl.DeviceIdType.MESH
F32 = jnp.float32
BF16 = jnp.bfloat16
LANES = 128
LOG2E = math.log2(math.e)


def mm(a, b):
    return jnp.dot(a, b, preferred_element_type=F32)


def mm_nt(a, b):
    return lax.dot_general(a, b, NT, preferred_element_type=F32)


def iota(shape, dim):
    return lax.broadcasted_iota(jnp.int32, shape, dim)


def partner(me, step, n):
    if n & (n - 1):
        return lax.rem(me + step, n)
    bits = [b for b in range(n.bit_length()) if step >> b & 1]
    return sum((1 - 2 * lax.rem(me // (1 << b), 2)) * (1 << b) for b in bits) + me


def far_first(n):
    return sorted(range(1, n), key=lambda step: (-(step >> 1).bit_count(), step & 1))


def split_pairs(values, odd):
    high = values.astype(BF16).astype(F32)
    return jnp.where(odd, values - high, high)


class Quads:
    def __init__(self, left, right, table, values, size):
        self.left, self.right, self.table, self.values, self.size = left, right, table, values, size
        self.stages = (self.scores, self.weights, self.mixed, self.turned)
        self.held = {}

    def scores(self, *unit):
        scores = mm(self.left(*unit), self.right(*unit))
        if self.table is not None:
            scores = scores + self.table(*unit)
        self.held[unit] = scores

    def weights(self, *unit):
        scores = self.held[unit]
        self.held[unit] = jnp.exp2((scores - jnp.max(scores, axis=0, keepdims=True)).astype(BF16))

    def mixed(self, *unit):
        self.held[unit] = mm(self.values(*unit), self.held[unit])

    def turned(self, *unit):
        mixed = self.held[unit]
        share = 1.0 / mixed[LANES:LANES + 1, :]
        parts = []
        for i in range(LANES // self.size):
            lane = slice(i // 2 * LANES, (i // 2 + 1) * LANES)
            parts.append(mixed[i * self.size:(i + 1) * self.size, lane] * share[:, lane])
        both = jnp.concatenate(parts, axis=0).T
        odd = lax.rem(iota((LANES // 2, LANES), 1) // self.size, 2) == 1
        self.held[unit] = jnp.where(odd, both[LANES // 2:], both[:LANES // 2])


class Pairs(Quads):
    def turned(self, b, h):
        mixed = self.held[b, h]
        share = 1.0 / mixed[2 * self.size:2 * self.size + 1, :]
        self.held[b, h] = jnp.concatenate(
            [mixed[:self.size, :LANES] * share[:, :LANES], mixed[self.size:2 * self.size, LANES:] * share[:, LANES:]],
            axis=0,
        )
        if h % 4 == 2:
            self.held[b, h] = jnp.concatenate([self.held.pop((b, h - 2)), self.held[b, h]], axis=0).T


def pair_of(queries_t, h, size):
    group = h // (LANES // size)
    blank = jnp.zeros((size, LANES), BF16)
    pieces = []
    for g in range(group * (LANES // size), (group + 1) * (LANES // size)):
        rows = queries_t[g * size:(g + 1) * size]
        pieces.append(jnp.concatenate([rows if g == h else blank, rows if g == h + 1 else blank], axis=1))
    return jnp.concatenate(pieces, axis=0)


def side_by_side(natural, turned, parity, group, size):
    lanes = iota((size, LANES), 1)
    keep = [(lanes < LANES // 2).astype(F32).astype(BF16), (lanes >= LANES // 2).astype(F32).astype(BF16)]
    blank = jnp.zeros((size, LANES), BF16)
    pieces = []
    for i in range(LANES // size):
        h = group * (LANES // size) + i
        rows = (natural if i % 2 == parity else turned)[h * size:(h + 1) * size] * keep[i % 2]
        pieces.append(jnp.concatenate([rows, blank] if i < 2 else [blank, rows], axis=1))
    return jnp.concatenate(pieces, axis=0)


def per_head(values, group, shape):
    lanes = iota(shape, 1) // (LANES // 2)
    out = jnp.broadcast_to(values[:, 4 * group:4 * group + 1], shape)
    for i in range(1, 4):
        out = jnp.where(lanes == i, values[:, 4 * group + i:4 * group + i + 1], out)
    return out


def root_mean(values):
    return lax.rsqrt(jnp.mean(values * values, axis=-1, keepdims=True) + 1e-06)


def halves_turned(rows):
    half = LANES // 2
    return jnp.concatenate([rows[(i ^ 1) * half:((i ^ 1) + 1) * half] for i in range(rows.shape[0] // half)], axis=0)


def staggered(stages, units, after):
    for step in range(len(units) + len(stages) - 1):
        for s, stage in enumerate(stages):
            if 0 <= step - s < len(units):
                stage(*units[step - s])
        if step >= len(stages) - 1:
            after(*units[step - len(stages) + 1])


def block_kernel(
    n_lon, n_lat, rows, width, depth, heads,
    fields_h, gain_lon_h, gain_lat_h, gain_mlp_h, temp_lon_h, bias_lon_h, temp_lat_h, bias_lat_h,
    ktab_h, qtab_h, wq1_h, wk1_h, wv1_h, wo1_h, wq2_h, wk2_h, wv2_h, wo2_h, wg_h, wu_h, wd_h,
    out,
    fields, gain_lon, gain_lat, gain_mlp, temp_lon, bias_lon, temp_lat, bias_lat,
    ktab, qtab, wq1, wk1, wv1, wo1, wq2, wk2, wv2, wo2, wg, wu, wd,
    norm_out, norm_in, field_out, field_in, att_out, att_in, upd_out,
    wqv1, wqv2, extra1, tables, resid, shuffle, hidden,
    local_sem, s1, r1, s2, r2, s3, r3, s4, r4, line_sem, plane_sem,
):
    me_lon = lax.axis_index("lon")
    me_lat = lax.axis_index("lat")
    total = n_lon * n_lat
    size = depth // heads
    cols = width // n_lat
    count = n_lat * rows
    cells = rows * width
    half = n_lat // 2
    block = half * rows
    side = me_lat // half
    own = lax.rem(me_lat, half)

    def lat_at(slot):
        if slot < half:
            return side * slot + (1 - side) * (n_lat - 1 - slot)
        return side * half + lax.rem(own + 1 + slot - half, half)

    def slot_of(lat, viewer):
        upper, seen = lat // half, viewer // half
        distant = upper + seen - 2 * upper * seen
        far_slot = upper * (n_lat - 1 - lat) + (1 - upper) * lat
        near_slot = half + lax.rem(lat + 2 * half - 1 - viewer + 2 * half * n_lat, half)
        return distant * far_slot + (1 - distant) * near_slot

    loads = {}

    def load(name, src, dst):
        loads[name] = pltpu.make_async_copy(src, dst, local_sem.at[len(loads)])
        loads[name].start()

    load("fields", fields_h, fields)
    load("gain_lon", gain_lon_h, gain_lon)
    barrier = pltpu.get_barrier_semaphore()
    order = far_first(n_lon)

    def signal_plane(sem):
        for step in order:
            pl.semaphore_signal(
                sem, inc=1, device_id=(partner(me_lon, step, n_lon), me_lat), device_id_type=MESH
            )

    other = partner(me_lon, 1, n_lon)

    def signal_line(sem, lons):
        @pl.when(me_lat > 0)
        def _():
            for lon in lons:
                pl.semaphore_signal(sem, inc=1, device_id=(lon, me_lat - 1), device_id_type=MESH)

        @pl.when(me_lat < n_lat - 1)
        def _():
            for lon in lons:
                pl.semaphore_signal(sem, inc=1, device_id=(lon, me_lat + 1), device_id_type=MESH)

    beside = jnp.minimum(me_lat, 1) + jnp.minimum(n_lat - 1 - me_lat, 1)
    signal_plane(barrier)
    signal_line(barrier, (me_lon, other))
    for slot in range(n_lat):
        load(f"ktab{slot}", ktab_h.at[lat_at(slot)], ktab.at[slot])
        load(f"qtab{slot}", qtab_h.at[lat_at(slot)], qtab.at[slot])
    for name, src, dst in [
        ("wq1", wq1_h, wq1), ("wk1", wk1_h, wk1), ("wv1", wv1_h, wv1), ("temp_lon", temp_lon_h, temp_lon),
        ("bias_lon", bias_lon_h, bias_lon), ("temp_lat", temp_lat_h, temp_lat), ("bias_lat", bias_lat_h, bias_lat),
        ("wo1", wo1_h, wo1), ("wq2", wq2_h, wq2), ("wk2", wk2_h, wk2), ("wv2", wv2_h, wv2), ("wo2", wo2_h, wo2),
        ("wg", wg_h, wg), ("wu", wu_h, wu), ("wd", wd_h, wd), ("gain_lat", gain_lat_h, gain_lat),
        ("gain_mlp", gain_mlp_h, gain_mlp),
    ]:
        load(name, src, dst)

    loads["fields"].wait()
    loads["gain_lon"].wait()
    wide = fields[...].astype(F32)
    factor = lax.rsqrt(jnp.mean(wide * wide, axis=-1, keepdims=True) + 1e-06)
    scaled = (wide * factor * gain_lon[...][None]).reshape(rows, n_lat, cols, depth).astype(BF16)
    pieces = wide.reshape(rows, n_lat, cols, depth).astype(BF16)
    for a in range(n_lat):
        norm_out[:, pl.ds(slot_of(a, me_lat), 1)] = scaled[:, a:a + 1]
        field_out[a] = pieces[:, a]

    pl.semaphore_wait(barrier, n_lon - 1 + 2 * beside)

    def my_cols(ref):
        return ref.at[:, pl.ds(pl.multiple_of(me_lat * cols, cols), cols), :]

    def send_norm(step):
        peer = partner(me_lon, step, n_lon)
        return pltpu.make_async_remote_copy(
            src_ref=norm_out.at[peer], dst_ref=norm_in.at[:, me_lon],
            send_sem=s1.at[0], recv_sem=r1.at[0], device_id=(peer, me_lat), device_id_type=MESH,
        )

    def send_field(peer):
        slot = slot_of(me_lat, peer)
        return pltpu.make_async_remote_copy(
            src_ref=field_out.at[peer], dst_ref=field_in.at[slot], send_sem=s2.at[0],
            recv_sem=r2.at[0], device_id=(other, peer), device_id_type=MESH,
        )

    def send_fields(hop):
        @pl.when(me_lat >= hop)
        def _():
            send_field(me_lat - hop).start()

        @pl.when(me_lat + hop < n_lat)
        def _():
            send_field(me_lat + hop).start()

    def whole(src, dst, sends, recvs):
        return pltpu.make_async_remote_copy(
            src_ref=src, dst_ref=dst, send_sem=sends, recv_sem=recvs,
            device_id=(me_lon, me_lat), device_id_type=MESH,
        )

    for step in order:
        send_norm(step).start()
    send_field(me_lat).start()
    signal_line(line_sem.at[0], (me_lon,))
    send_fields(1)
    norm_in[:, pl.ds(me_lon, 1)] = norm_out[pl.ds(me_lon, 1)].reshape(n_lat, 1, cols, depth)

    for name in ["wq1", "wk1", "wv1", "temp_lon", "bias_lon", "temp_lat", "bias_lat"] + [
        f"{kind}{slot}" for slot in range(n_lat) for kind in ("ktab", "qtab")
    ]:
        loads[name].wait()
    wqv1[:depth] = wq1[...].T
    wqv1[depth:] = wv1[...].T
    groups = depth // LANES
    shape = (16, 2 * LANES)
    odd = lax.rem(iota(shape, 0), 2) == 1
    halves = iota((16, LANES), 1) < LANES // 2
    for b in range(2):
        wave = jnp.where(halves, qtab[2 * b], qtab[2 * b + 1])
        wave = jnp.concatenate([wave, wave], axis=1)
        for h in range(0, heads, 2):
            weight = jnp.where(
                iota(shape, 1) < LANES, bias_lon[:, h:h + 1], bias_lon[:, h + 1:h + 2]
            ) * LOG2E
            extra1[b, h // 2] = split_pairs(weight * wave, odd).astype(BF16)
    hold = half * rows
    shape = (LANES, 2 * LANES)
    key_cell, query_cell = iota(shape, 0), lax.rem(iota(shape, 1), LANES // 2)

    def lat_value(spot, distant):
        group = spot // rows
        value = jnp.zeros(shape, jnp.int32)
        for g in range(half):
            value = jnp.where(group == g, lat_at(g if distant else half + g), value)
        return value * rows + lax.rem(spot, rows)

    key_far, key_near = lat_value(lax.rem(key_cell, hold), True), lat_value(lax.rem(key_cell, hold), False)
    same = lax.rem(key_cell, LANES // 2) // hold == query_cell // hold
    for g in range(groups):
        weight = per_head(bias_lat, g, shape) * (LOG2E / count)
        for f in range(2):
            there = lat_value(lax.rem(query_cell, hold), f == 0)
            for c in range(2):
                first_part = key_cell < LANES // 2
                here = jnp.where(first_part, key_far, key_near) if c == 0 else jnp.where(first_part, key_near, key_far)
                tables[f, c, g] = jnp.where(same, weight * jnp.abs(here - there).astype(F32), -1e30)

    pl.semaphore_wait(line_sem.at[0], beside)

    @pl.when(me_lat == 1)
    def _():
        pl.semaphore_signal(line_sem.at[1], inc=1, device_id=(me_lon, me_lat - 1), device_id_type=MESH)

    @pl.when(me_lat == n_lat - 2)
    def _():
        pl.semaphore_signal(line_sem.at[1], inc=1, device_id=(me_lon, me_lat + 1), device_id_type=MESH)

    send_fields(2)

    @pl.when(beside < 2)
    def _():
        pl.semaphore_wait(line_sem.at[1], 1)

    signal_plane(plane_sem)
    send_fields(3)

    def scales(temp):
        return [jnp.broadcast_to(temp[:, h:h + 1] * (LOG2E / math.sqrt(size)), (size, LANES)) for h in range(heads)]

    def scaled_t(queries_t, temp):
        factors = [jnp.concatenate([one] * (queries_t.shape[1] // LANES), axis=1) for one in temp]
        return (queries_t * jnp.concatenate(factors, axis=0)).astype(BF16)

    scale_lon = scales(temp_lon)
    norm_all = whole(norm_out.at[pl.ds(0, n_lon - 1)], norm_out.at[pl.ds(0, n_lon - 1)], s1.at[0], r1.at[0])
    norm_all.wait_recv()

    nlon = n_lon * width
    normed = norm_in[...].reshape(nlon, depth)
    keys = mm(normed, wk1[...]).astype(BF16)
    both_t = mm_nt(wqv1[...], normed)
    queries_t = scaled_t(both_t[:depth], scale_lon)
    values_t = both_t[depth:].astype(BF16)
    key_extra = ktab[...].reshape(nlon, LANES)[:, :16]
    ones = jnp.ones((16, nlon), BF16)

    row_work = Pairs(
        lambda b, h: jnp.concatenate([keys[:, h // 4 * LANES:(h // 4 + 1) * LANES], key_extra], axis=1),
        lambda b, h: jnp.concatenate(
            [pair_of(queries_t[:, b * LANES:(b + 1) * LANES], h, size), extra1[b, h // 2]], axis=0
        ),
        None,
        lambda b, h: jnp.concatenate([values_t[h * size:(h + 2) * size], ones], axis=0),
        size,
    )

    distant_slot = slot_of(me_lat, (1 - side) * half)

    def send_att(slot, peer):
        group = distant_slot if slot < half else half + (n_lat - 2 - slot) % half
        return pltpu.make_async_remote_copy(
            src_ref=att_out.at[slot * n_lon + partner(peer, 1, n_lon)], dst_ref=att_in.at[group * rows + me_lon], send_sem=s3.at[0],
            recv_sem=r3.at[min(slot // half, 1)], device_id=(peer, lat_at(slot)), device_id_type=MESH,
        )

    def row_done(b, h):
        if h < heads - 2:
            return
        att = jnp.concatenate([row_work.held.pop((b, k)) for k in range(2, heads, 4)], axis=1)
        att_out[b * half * n_lon:(b + 1) * half * n_lon] = att.reshape(half * n_lon, cols, depth).astype(BF16)
        if b == 0:
            pl.semaphore_wait(plane_sem, n_lon - 1)
        for hop in order + [0]:
            for slot in range(b * half, (b + 1) * half):
                if hop or slot < n_lat - 1:
                    send_att(slot, partner(me_lon, hop, n_lon)).start()

    staggered(row_work.stages, [(b, h) for b in range(2) for h in range(0, heads, 2)], row_done)
    att_in[pl.ds((n_lat - 1) * rows + me_lon, 1)] = att_out[pl.ds((n_lat - 1) * n_lon + other, 1)]

    for name in ("wo1", "wq2", "wk2", "wv2", "wo2", "wg", "wu", "wd", "gain_lat", "gain_mlp"):
        loads[name].wait()
    wqv2[:depth] = wq2[...].T
    wqv2[depth:] = wv2[...].T
    scale_lat = scales(temp_lat)
    field_all = whole(field_out, field_in, s2.at[0], r2.at[0])
    field_all.wait_recv()

    near_all = whole(att_out.at[pl.ds(0, count // 2 - 1)], att_in.at[pl.ds(0, count // 2 - 1)], s3.at[0], r3.at[1])
    far_all = whole(att_out.at[pl.ds(0, count // 2)], att_in.at[pl.ds(0, count // 2)], s3.at[0], r3.at[0])
    att_all = whole(att_out.at[pl.ds(0, total - 1)], att_in.at[pl.ds(0, total - 1)], s3.at[0], r3.at[0])
    starts = [list(range(cols)), list(range(cols // 2, cols)) + list(range(cols // 2))]

    def by_column(f, values):
        values = values.astype(F32).reshape(LANES, depth)
        parts = []
        for g in range(groups):
            shuffle[groups * f + g] = values[:, g * LANES:(g + 1) * LANES]
            parts.append([shuffle[groups * f + g, pl.ds(c, block, stride=cols), :] for c in starts[f]])
        return jnp.concatenate([jnp.concatenate(part, axis=0) for part in parts], axis=1)

    for f in range(2):
        resid[f * LANES:(f + 1) * LANES] = by_column(f, field_in[f * half:(f + 1) * half])

    firsts, keys2, queries2, turned2, values2 = {}, {}, {}, {}, {}

    def project_columns(f):
        attended = by_column(f, att_in[f * block:(f + 1) * block]).astype(BF16)
        firsts[f] = resid[f * LANES:(f + 1) * LANES] + mm(attended, wo1[...])
        gained = (firsts[f] * gain_lat[...]).astype(BF16)
        factor = root_mean(firsts[f])
        across = jnp.broadcast_to(factor, (LANES, LANES)).T[:1]
        turned = jnp.broadcast_to(halves_turned(factor), (LANES, LANES)).T[:1]
        keys2[f] = (mm(gained, wk2[...]) * factor).astype(BF16)
        both_t = mm_nt(wqv2[...], gained)
        queries2[f] = scaled_t(both_t[:depth], [one * across for one in scale_lat])
        turned2[f] = scaled_t(mm_nt(wqv2[:depth], halves_turned(gained)), [one * turned for one in scale_lat])
        values2[f] = (both_t[depth:] * across).astype(BF16)

    far_all.wait_recv()
    project_columns(0)
    near_all.wait_recv()
    project_columns(1)
    part = LANES // 2
    low = (iota((LANES, LANES), 1) < part).astype(F32).astype(BF16)
    high = (iota((LANES, LANES), 1) >= part).astype(F32).astype(BF16)
    ones = jnp.ones((16, LANES), BF16)

    def column_keys(f, c, g):
        lane = slice(g * LANES, (g + 1) * LANES)
        return jnp.concatenate([keys2[c][:part, lane], keys2[1 - c][part:, lane]], axis=0)

    def column_values(f, c, g):
        row = slice(g * LANES, (g + 1) * LANES)
        return jnp.concatenate([values2[c][row] * low + values2[1 - c][row] * high, ones], axis=0)

    col_work = Quads(
        column_keys,
        lambda f, c, g: side_by_side(queries2[f], turned2[f], c if f == 0 else 1 - c, g, size),
        lambda f, c, g: tables[f, c, g],
        column_values,
        size,
    )
    ff = wg.shape[1]
    step_ff = min(ff, 256)

    def send_upd(slot):
        return pltpu.make_async_remote_copy(
            src_ref=upd_out.at[slot], dst_ref=my_cols(out), send_sem=s4.at[0], recv_sem=r4.at[0],
            device_id=(other, lat_at(slot)), device_id_type=MESH,
        )

    def col_done(f, c, g):
        if c != (1 if f == 0 else 0) or g < groups - 1:
            return
        att = jnp.concatenate(
            [jnp.concatenate([col_work.held.pop((f, k, g)) for g in range(groups)], axis=1)
             for k in ((0, 1) if f == 0 else (1, 0))], axis=0
        )
        second = firsts[f] + mm(att.astype(BF16), wo2[...])
        gained = (second * gain_mlp[...]).astype(BF16)
        factor = root_mean(second)
        for k in range(0, ff, step_ff):
            gate = mm(gained, wg[:, k:k + step_ff])
            upper = mm(gained, wu[:, k:k + step_ff])
            hidden[:, k:k + step_ff] = (gate * upper * (jnp.tanh(gate * (0.5 * factor)) + 1.0)).astype(BF16)
        second = second + (0.5 * factor * factor) * mm(hidden[...], wd[...])
        for i, c in enumerate(starts[f]):
            for g in range(groups):
                shuffle[groups * f + g, pl.ds(c, block, stride=cols), :] = (
                    second[i * block:(i + 1) * block, g * LANES:(g + 1) * LANES]
                )
        updated = jnp.concatenate([shuffle[groups * f + g] for g in range(groups)], axis=1)
        upd_out[f * half:(f + 1) * half] = updated.reshape(half, rows, cols, depth).astype(BF16)
        for slot in range(f * half, (f + 1) * half):
            send_upd(slot).start()

    for f in range(2):
        staggered(
            col_work.stages, [(f, c, g) for c in ((0, 1) if f == 0 else (1, 0)) for g in range(groups)], col_done
        )
    norm_all.wait_send()
    field_all.wait_send()
    att_all.wait_send()
    upd_all = whole(upd_out, upd_out, s4.at[0], r4.at[0])
    upd_all.wait_send()
    upd_all.wait_recv()


def fused_body(
    fields, norm_lon, query_lon, key_lon, value_lon, out_lon, temp_lon, bias_lon,
    norm_lat, query_lat, key_lat, value_lat, out_lat, temp_lat, bias_lat,
    norm_mlp, w_gate, w_up, w_down,
):
    rows, width, depth = fields.shape
    heads = temp_lon.shape[0]
    n_lon, n_lat = lax.axis_size("lon"), lax.axis_size("lat")
    cols = width // n_lat
    nlon = width * n_lon
    total = n_lon * n_lat
    cells = rows * width
    place = np.arange(nlon).reshape(n_lon, n_lat, cols).transpose(1, 0, 2).reshape(nlon)
    turn = place * (2.0 * math.pi / nlon)
    waves = np.stack([np.cos(turn)] * 4 + [np.sin(turn)] * 4, axis=1).astype(np.float32)
    high = waves.astype(jnp.bfloat16).astype(np.float32)
    ktab = np.zeros((nlon, LANES), np.float32)
    ktab[:, :8] = np.where(np.arange(8)[None] % 4 < 2, high, waves - high)
    ktab = ktab.astype(jnp.bfloat16).reshape(n_lat, n_lon * cols, LANES)
    qtab = np.zeros((n_lat, 16, LANES), np.float32)
    qtab[:, :8] = np.tile(waves.reshape(n_lat, LANES // 2, 8).transpose(0, 2, 1), (1, 1, 2))
    hbm = pl.BlockSpec(memory_space=pl.ANY)
    weights = (query_lon, key_lon, value_lon, out_lon, query_lat, key_lat, value_lat, out_lat,
               w_gate, w_up, w_down)
    dma = pltpu.SemaphoreType.DMA
    updated = pl.pallas_call(
        functools.partial(block_kernel, n_lon, n_lat, rows, width, depth, heads),
        out_shape=pltpu.VMEM((rows, width, depth), BF16),
        in_specs=[hbm] * 21,
        out_specs=hbm,
        scratch_shapes=[pltpu.VMEM((rows, width, depth), BF16)]
        + [pltpu.VMEM((1, depth), F32)] * 3
        + [pltpu.VMEM((1, heads), F32)] * 4
        + [pltpu.VMEM(ktab.shape, BF16), pltpu.VMEM(qtab.shape, F32)]
        + [pltpu.VMEM(w.shape, w.dtype) for w in weights]
        + [
            pltpu.VMEM((rows, n_lat, cols, depth), BF16),
            pltpu.VMEM((n_lat, n_lon, cols, depth), BF16),
            pltpu.VMEM((n_lat, rows, cols, depth), BF16),
            pltpu.VMEM((n_lat, rows, cols, depth), BF16),
            pltpu.VMEM((total, cols, depth), BF16),
            pltpu.VMEM((n_lat * rows, cols, depth), BF16),
            pltpu.VMEM((n_lat, rows, cols, depth), BF16),
            pltpu.VMEM((2 * depth, depth), BF16),
            pltpu.VMEM((2 * depth, depth), BF16),
            pltpu.VMEM((2, heads // 2, 16, 2 * LANES), BF16),
            pltpu.VMEM((2, 2, depth // LANES, LANES, 2 * LANES), F32),
            pltpu.VMEM((cells, depth), F32),
            pltpu.VMEM((2 * depth // LANES, LANES, LANES), F32),
            pltpu.VMEM((LANES, w_gate.shape[1]), BF16),
            dma((32,)),
            dma((1,)), dma((1,)),
            dma((1,)), dma((1,)),
            dma((1,)), dma((2,)),
            dma((1,)), dma((1,)),
            pltpu.SemaphoreType.REGULAR((2,)),
            pltpu.SemaphoreType.REGULAR,
        ],
        compiler_params=pltpu.CompilerParams(collective_id=0, has_side_effects=True),
    )(
        fields, norm_lon[None], norm_lat[None], norm_mlp[None], temp_lon[None], bias_lon[None],
        temp_lat[None], bias_lat[None],
        jnp.asarray(ktab), jnp.asarray(qtab), *weights,
    )
    return updated


def fits(rows, width, n_lon, n_lat, heads, depth):
    return (
        rows == n_lon and n_lat % 2 == 0 and width == 8 * n_lat and rows * width == 2 * LANES
        and width * n_lon == 2 * LANES and n_lat == 4 and depth % LANES == 0 and heads * LANES == 4 * depth
    )


def choose(*args):
    rows, width, _ = args[0].shape
    n_lon, n_lat = lax.axis_size("lon"), lax.axis_size("lat")
    if fits(rows, width, n_lon, n_lat, args[6].shape[0], args[0].shape[2]):
        return fused_body(*args)
    return body(*args)


def solution(mesh):
    in_specs = (P("lat", "lon", None),) + (P(),) * 18
    out_specs = P("lat", "lon", None)
    return jax.shard_map(choose, mesh=mesh, in_specs=in_specs, out_specs=out_specs, check_vma=False)
```

```python
import math

import jax
import jax.numpy as jnp
import functools
import numpy as np
from jax import lax
from jax.experimental import pallas as pl
from jax.experimental.pallas import tpu as pltpu
from jax.sharding import PartitionSpec as P


def normalize(values, gain):
    factor = lax.rsqrt(jnp.mean(values * values, axis=-1, keepdims=True) + 1e-06)
    return (values * factor * gain).astype(jnp.bfloat16)


def project(values, weight):
    return jnp.dot(values, weight, preferred_element_type=jnp.float32).astype(jnp.bfloat16)


def attend_lat(queries, keys, values, temp, bias):
    count, cols, depth = queries.shape
    heads = temp.shape[0]
    size = depth // heads
    qh = queries.reshape(count, cols, heads, size)
    kh = keys.reshape(count, cols, heads, size)
    vh = values.reshape(count, cols, heads, size)
    scores = jnp.einsum("ichd,jchd->chij", qh, kh, preferred_element_type=jnp.float32)
    place = jnp.arange(count, dtype=jnp.int32)
    spread = jnp.abs(place[:, None] - place[None, :]).astype(jnp.float32) / count
    scores = (
        scores * (temp / math.sqrt(size))[None, :, None, None]
        + bias[None, :, None, None] * spread[None, None]
    )
    expo = jnp.exp(scores - jnp.max(scores, axis=-1, keepdims=True))
    denom = jnp.sum(expo, axis=-1)
    mixed = jnp.einsum(
        "chij,jchd->ichd", expo.astype(jnp.bfloat16), vh, preferred_element_type=jnp.float32
    )
    mixed = mixed / jnp.transpose(denom, (2, 0, 1))[..., None]
    return mixed.astype(jnp.bfloat16).reshape(count, cols, depth)


def body(
    fields,
    norm_lon,
    query_lon,
    key_lon,
    value_lon,
    out_lon,
    temp_lon,
    bias_lon,
    norm_lat,
    query_lat,
    key_lat,
    value_lat,
    out_lat,
    temp_lat,
    bias_lat,
    norm_mlp,
    w_gate,
    w_up,
    w_down,
):
    rows, width, depth = fields.shape
    heads = temp_lon.shape[0]
    size = depth // heads
    total_lon = width * lax.axis_size("lon")
    resid = fields.astype(jnp.float32)
    normed = normalize(resid, norm_lon)
    scale_lon = temp_lon / math.sqrt(size)
    query_place = lax.axis_index("lon") * width + jnp.arange(width, dtype=jnp.int32)
    queries = project(normed, query_lon).reshape(rows, width, heads, size)
    piece = lax.all_gather(normed, "lon", axis=1, tiled=True)
    keys = project(piece, key_lon)
    count = keys.shape[1]
    key_place = jnp.arange(count, dtype=jnp.int32)
    angle = (query_place[:, None] - key_place[None, :]).astype(jnp.float32) * (
        2.0 * math.pi / total_lon
    )
    wave = jnp.cos(angle)

    def one_row(items):
        query_row, key_row, value_row, peak, total, accum = items
        key_heads = key_row.reshape(count, heads, size)
        value_heads = value_row.reshape(count, heads, size)
        scores = jnp.einsum(
            "ihd,jhd->hij", query_row, key_heads, preferred_element_type=jnp.float32
        )
        scores = scores * scale_lon[:, None, None] + bias_lon[:, None, None] * wave[None]
        fresh = jnp.maximum(peak, jnp.max(scores, axis=-1))
        shrink = jnp.exp(peak - fresh)
        expo = jnp.exp(scores - fresh[..., None])
        total = total * shrink + jnp.sum(expo, axis=-1)
        mixed = jnp.einsum(
            "hij,jhd->ihd",
            expo.astype(jnp.bfloat16),
            value_heads,
            preferred_element_type=jnp.float32,
        )
        accum = accum.reshape(width, heads, size) * jnp.transpose(shrink)[:, :, None] + mixed
        return (fresh, total, accum.reshape(width, depth))

    peak = jnp.full((rows, heads, width), -1e30, jnp.float32)
    total = jnp.zeros((rows, heads, width), jnp.float32)
    accum = jnp.zeros((rows, width, depth), jnp.float32)
    peak, total, accum = lax.map(
        one_row, (queries, keys, project(piece, value_lon), peak, total, accum)
    )
    attended = accum.reshape(rows, width, heads, size) / jnp.transpose(total, (0, 2, 1))[..., None]
    attended = attended.astype(jnp.bfloat16).reshape(rows, width, depth)
    first = resid + jnp.dot(attended, out_lon, preferred_element_type=jnp.float32)
    normed_lat = normalize(first, norm_lat)
    query_col = project(normed_lat, query_lat)
    key_col = project(normed_lat, key_lat)
    value_col = project(normed_lat, value_lat)
    query_col, key_col, value_col = (
        lax.all_to_all(query_col, "lat", split_axis=1, concat_axis=0, tiled=True),
        lax.all_to_all(key_col, "lat", split_axis=1, concat_axis=0, tiled=True),
        lax.all_to_all(value_col, "lat", split_axis=1, concat_axis=0, tiled=True),
    )
    mixed_lat = attend_lat(query_col, key_col, value_col, temp_lat, bias_lat)
    returned = lax.all_to_all(mixed_lat, "lat", split_axis=0, concat_axis=1, tiled=True)
    second = first + jnp.dot(returned, out_lat, preferred_element_type=jnp.float32)
    normed_mlp = normalize(second, norm_mlp)
    gate = jnp.dot(normed_mlp, w_gate, preferred_element_type=jnp.float32)
    upper = jnp.dot(normed_mlp, w_up, preferred_element_type=jnp.float32)
    hidden = (jax.nn.silu(gate) * upper).astype(jnp.bfloat16)
    return (second + jnp.dot(hidden, w_down, preferred_element_type=jnp.float32)).astype(
        jnp.bfloat16
    )


NT = (((1,), (1,)), ((), ()))
MESH = pl.DeviceIdType.MESH
F32 = jnp.float32
BF16 = jnp.bfloat16
LANES = 128
LOG2E = math.log2(math.e)


def mm(a, b):
    return jnp.dot(a, b, preferred_element_type=F32)


def mm_nt(a, b):
    return lax.dot_general(a, b, NT, preferred_element_type=F32)


def iota(shape, dim):
    return lax.broadcasted_iota(jnp.int32, shape, dim)


def partner(me, step, n):
    if n & (n - 1):
        return lax.rem(me + step, n)
    bits = [b for b in range(n.bit_length()) if step >> b & 1]
    return sum((1 - 2 * lax.rem(me // (1 << b), 2)) * (1 << b) for b in bits) + me


def far_first(n):
    return sorted(range(1, n), key=lambda step: (-(step >> 1).bit_count(), step & 1))


def split_pairs(values, odd):
    high = values.astype(BF16).astype(F32)
    return jnp.where(odd, values - high, high)


class Quads:
    def __init__(self, left, right, table, values, size):
        self.left, self.right, self.table, self.values, self.size = left, right, table, values, size
        self.stages = (self.scores, self.weights, self.mixed, self.turned)
        self.held = {}

    def scores(self, *unit):
        scores = mm(self.left(*unit), self.right(*unit))
        if self.table is not None:
            scores = scores + self.table(*unit)
        self.held[unit] = scores

    def weights(self, *unit):
        scores = self.held[unit]
        self.held[unit] = jnp.exp2((scores - jnp.max(scores, axis=0, keepdims=True)).astype(BF16))

    def mixed(self, *unit):
        self.held[unit] = mm(self.values(*unit), self.held[unit])

    def turned(self, *unit):
        mixed = self.held[unit]
        share = 1.0 / mixed[LANES:LANES + 1, :]
        parts = []
        for i in range(LANES // self.size):
            lane = slice(i // 2 * LANES, (i // 2 + 1) * LANES)
            parts.append(mixed[i * self.size:(i + 1) * self.size, lane] * share[:, lane])
        both = jnp.concatenate(parts, axis=0).T
        odd = lax.rem(iota((LANES // 2, LANES), 1) // self.size, 2) == 1
        self.held[unit] = jnp.where(odd, both[LANES // 2:], both[:LANES // 2])


class Pairs(Quads):
    def turned(self, b, h):
        mixed = self.held[b, h]
        share = 1.0 / mixed[2 * self.size:2 * self.size + 1, :]
        self.held[b, h] = jnp.concatenate(
            [mixed[:self.size, :LANES] * share[:, :LANES], mixed[self.size:2 * self.size, LANES:] * share[:, LANES:]],
            axis=0,
        )
        if h % 4 == 2:
            self.held[b, h] = jnp.concatenate([self.held.pop((b, h - 2)), self.held[b, h]], axis=0).T


def pair_of(queries_t, h, size):
    group = h // (LANES // size)
    blank = jnp.zeros((size, LANES), BF16)
    pieces = []
    for g in range(group * (LANES // size), (group + 1) * (LANES // size)):
        rows = queries_t[g * size:(g + 1) * size]
        pieces.append(jnp.concatenate([rows if g == h else blank, rows if g == h + 1 else blank], axis=1))
    return jnp.concatenate(pieces, axis=0)


def side_by_side(natural, turned, parity, group, size):
    lanes = iota((size, LANES), 1)
    keep = [(lanes < LANES // 2).astype(F32).astype(BF16), (lanes >= LANES // 2).astype(F32).astype(BF16)]
    blank = jnp.zeros((size, LANES), BF16)
    pieces = []
    for i in range(LANES // size):
        h = group * (LANES // size) + i
        rows = (natural if i % 2 == parity else turned)[h * size:(h + 1) * size] * keep[i % 2]
        pieces.append(jnp.concatenate([rows, blank] if i < 2 else [blank, rows], axis=1))
    return jnp.concatenate(pieces, axis=0)


def per_head(values, group, shape):
    lanes = iota(shape, 1) // (LANES // 2)
    out = jnp.broadcast_to(values[:, 4 * group:4 * group + 1], shape)
    for i in range(1, 4):
        out = jnp.where(lanes == i, values[:, 4 * group + i:4 * group + i + 1], out)
    return out


def root_mean(values):
    return lax.rsqrt(jnp.mean(values * values, axis=-1, keepdims=True) + 1e-06)


def halves_turned(rows):
    half = LANES // 2
    return jnp.concatenate([rows[(i ^ 1) * half:((i ^ 1) + 1) * half] for i in range(rows.shape[0] // half)], axis=0)


def staggered(stages, units, after):
    for step in range(len(units) + len(stages) - 1):
        for s, stage in enumerate(stages):
            if 0 <= step - s < len(units):
                stage(*units[step - s])
        if step >= len(stages) - 1:
            after(*units[step - len(stages) + 1])


def block_kernel(
    n_lon, n_lat, rows, width, depth, heads,
    fields_h, gain_lon_h, gain_lat_h, gain_mlp_h, temp_lon_h, bias_lon_h, temp_lat_h, bias_lat_h,
    ktab_h, qtab_h, wq1_h, wk1_h, wv1_h, wo1_h, wq2_h, wk2_h, wv2_h, wo2_h, wg_h, wu_h, wd_h,
    out,
    fields, gain_lon, gain_lat, gain_mlp, temp_lon, bias_lon, temp_lat, bias_lat,
    ktab, qtab, wq1, wk1, wv1, wo1, wq2, wk2, wv2, wo2, wg, wu, wd,
    norm_out, norm_in, field_out, field_in, att_out, att_in, upd_out,
    wqv1, wqv2, extra1, tables, resid, shuffle, hidden,
    local_sem, s1, r1, s2, r2, s3, r3, s4, r4, line_sem, plane_sem,
):
    me_lon = lax.axis_index("lon")
    me_lat = lax.axis_index("lat")
    total = n_lon * n_lat
    size = depth // heads
    cols = width // n_lat
    count = n_lat * rows
    cells = rows * width
    half = n_lat // 2
    block = half * rows
    side = me_lat // half
    own = lax.rem(me_lat, half)

    def lat_at(slot):
        if slot < half:
            return side * slot + (1 - side) * (n_lat - 1 - slot)
        return side * half + lax.rem(own + 1 + slot - half, half)

    def slot_of(lat, viewer):
        upper, seen = lat // half, viewer // half
        distant = upper + seen - 2 * upper * seen
        far_slot = upper * (n_lat - 1 - lat) + (1 - upper) * lat
        near_slot = half + lax.rem(lat + 2 * half - 1 - viewer + 2 * half * n_lat, half)
        return distant * far_slot + (1 - distant) * near_slot

    loads = {}

    def load(name, src, dst):
        loads[name] = pltpu.make_async_copy(src, dst, local_sem.at[len(loads)])
        loads[name].start()

    load("fields", fields_h, fields)
    load("gain_lon", gain_lon_h, gain_lon)
    barrier = pltpu.get_barrier_semaphore()
    order = far_first(n_lon)

    def signal_plane(sem):
        for step in order:
            pl.semaphore_signal(
                sem, inc=1, device_id=(partner(me_lon, step, n_lon), me_lat), device_id_type=MESH
            )

    other = partner(me_lon, 1, n_lon)

    def signal_line(sem, lons):
        @pl.when(me_lat > 0)
        def _():
            for lon in lons:
                pl.semaphore_signal(sem, inc=1, device_id=(lon, me_lat - 1), device_id_type=MESH)

        @pl.when(me_lat < n_lat - 1)
        def _():
            for lon in lons:
                pl.semaphore_signal(sem, inc=1, device_id=(lon, me_lat + 1), device_id_type=MESH)

    beside = jnp.minimum(me_lat, 1) + jnp.minimum(n_lat - 1 - me_lat, 1)
    signal_plane(barrier)
    signal_line(barrier, (me_lon, other))
    for slot in range(n_lat):
        load(f"ktab{slot}", ktab_h.at[lat_at(slot)], ktab.at[slot])
        load(f"qtab{slot}", qtab_h.at[lat_at(slot)], qtab.at[slot])
    for name, src, dst in [
        ("wq1", wq1_h, wq1), ("wk1", wk1_h, wk1), ("wv1", wv1_h, wv1), ("temp_lon", temp_lon_h, temp_lon),
        ("bias_lon", bias_lon_h, bias_lon), ("temp_lat", temp_lat_h, temp_lat), ("bias_lat", bias_lat_h, bias_lat),
        ("wo1", wo1_h, wo1), ("wq2", wq2_h, wq2), ("wk2", wk2_h, wk2), ("wv2", wv2_h, wv2), ("wo2", wo2_h, wo2),
        ("wg", wg_h, wg), ("wu", wu_h, wu), ("wd", wd_h, wd), ("gain_lat", gain_lat_h, gain_lat),
        ("gain_mlp", gain_mlp_h, gain_mlp),
    ]:
        load(name, src, dst)

    loads["fields"].wait()
    loads["gain_lon"].wait()
    wide = fields[...].astype(F32)
    factor = lax.rsqrt(jnp.mean(wide * wide, axis=-1, keepdims=True) + 1e-06)
    scaled = (wide * factor * gain_lon[...][None]).reshape(rows, n_lat, cols, depth).astype(BF16)
    pieces = wide.reshape(rows, n_lat, cols, depth).astype(BF16)
    for a in range(n_lat):
        norm_out[:, pl.ds(slot_of(a, me_lat), 1)] = scaled[:, a:a + 1]
        field_out[a] = pieces[:, a]

    pl.semaphore_wait(barrier, n_lon - 1 + 2 * beside)

    def my_cols(ref):
        return ref.at[:, pl.ds(pl.multiple_of(me_lat * cols, cols), cols), :]

    def send_norm(step):
        peer = partner(me_lon, step, n_lon)
        return pltpu.make_async_remote_copy(
            src_ref=norm_out.at[peer], dst_ref=norm_in.at[:, me_lon],
            send_sem=s1.at[0], recv_sem=r1.at[0], device_id=(peer, me_lat), device_id_type=MESH,
        )

    def send_field(peer):
        slot = slot_of(me_lat, peer)
        return pltpu.make_async_remote_copy(
            src_ref=field_out.at[peer], dst_ref=field_in.at[slot], send_sem=s2.at[0],
            recv_sem=r2.at[0], device_id=(other, peer), device_id_type=MESH,
        )

    def send_fields(hop):
        @pl.when(me_lat >= hop)
        def _():
            send_field(me_lat - hop).start()

        @pl.when(me_lat + hop < n_lat)
        def _():
            send_field(me_lat + hop).start()

    def whole(src, dst, sends, recvs):
        return pltpu.make_async_remote_copy(
            src_ref=src, dst_ref=dst, send_sem=sends, recv_sem=recvs,
            device_id=(me_lon, me_lat), device_id_type=MESH,
        )

    for step in order:
        send_norm(step).start()
    send_field(me_lat).start()
    signal_line(line_sem.at[0], (me_lon,))
    send_fields(1)
    norm_in[:, pl.ds(me_lon, 1)] = norm_out[pl.ds(me_lon, 1)].reshape(n_lat, 1, cols, depth)

    for name in ["wq1", "wk1", "wv1", "temp_lon", "bias_lon", "temp_lat", "bias_lat"] + [
        f"{kind}{slot}" for slot in range(n_lat) for kind in ("ktab", "qtab")
    ]:
        loads[name].wait()
    wqv1[:depth] = wq1[...].T
    wqv1[depth:] = wv1[...].T
    groups = depth // LANES
    shape = (16, 2 * LANES)
    odd = lax.rem(iota(shape, 0), 2) == 1
    halves = iota((16, LANES), 1) < LANES // 2
    for b in range(2):
        wave = jnp.where(halves, qtab[2 * b], qtab[2 * b + 1])
        wave = jnp.concatenate([wave, wave], axis=1)
        for h in range(0, heads, 2):
            weight = jnp.where(
                iota(shape, 1) < LANES, bias_lon[:, h:h + 1], bias_lon[:, h + 1:h + 2]
            ) * LOG2E
            extra1[b, h // 2] = split_pairs(weight * wave, odd).astype(BF16)
    hold = half * rows
    shape = (LANES, 2 * LANES)
    key_cell, query_cell = iota(shape, 0), lax.rem(iota(shape, 1), LANES // 2)

    def lat_value(spot, distant):
        group = spot // rows
        value = jnp.zeros(shape, jnp.int32)
        for g in range(half):
            value = jnp.where(group == g, lat_at(g if distant else half + g), value)
        return value * rows + lax.rem(spot, rows)

    key_far, key_near = lat_value(lax.rem(key_cell, hold), True), lat_value(lax.rem(key_cell, hold), False)
    same = lax.rem(key_cell, LANES // 2) // hold == query_cell // hold
    for g in range(groups):
        weight = per_head(bias_lat, g, shape) * (LOG2E / count)
        for f in range(2):
            there = lat_value(lax.rem(query_cell, hold), f == 0)
            for c in range(2):
                first_part = key_cell < LANES // 2
                here = jnp.where(first_part, key_far, key_near) if c == 0 else jnp.where(first_part, key_near, key_far)
                tables[f, c, g] = jnp.where(same, weight * jnp.abs(here - there).astype(F32), -1e30)

    pl.semaphore_wait(line_sem.at[0], beside)

    @pl.when(me_lat == 1)
    def _():
        pl.semaphore_signal(line_sem.at[1], inc=1, device_id=(me_lon, me_lat - 1), device_id_type=MESH)

    @pl.when(me_lat == n_lat - 2)
    def _():
        pl.semaphore_signal(line_sem.at[1], inc=1, device_id=(me_lon, me_lat + 1), device_id_type=MESH)

    send_fields(2)

    @pl.when(beside < 2)
    def _():
        pl.semaphore_wait(line_sem.at[1], 1)

    signal_plane(plane_sem)
    send_fields(3)

    def scales(temp):
        return [jnp.broadcast_to(temp[:, h:h + 1] * (LOG2E / math.sqrt(size)), (size, LANES)) for h in range(heads)]

    def scaled_t(queries_t, temp):
        factors = [jnp.concatenate([one] * (queries_t.shape[1] // LANES), axis=1) for one in temp]
        return (queries_t * jnp.concatenate(factors, axis=0)).astype(BF16)

    scale_lon = scales(temp_lon)
    norm_all = whole(norm_out.at[pl.ds(0, n_lon - 1)], norm_out.at[pl.ds(0, n_lon - 1)], s1.at[0], r1.at[0])
    norm_all.wait_recv()

    nlon = n_lon * width
    normed = norm_in[...].reshape(nlon, depth)
    keys = mm(normed, wk1[...]).astype(BF16)
    both_t = mm_nt(wqv1[...], normed)
    queries_t = scaled_t(both_t[:depth], scale_lon)
    values_t = both_t[depth:].astype(BF16)
    key_extra = ktab[...].reshape(nlon, LANES)[:, :16]
    ones = jnp.ones((16, nlon), BF16)

    row_work = Pairs(
        lambda b, h: jnp.concatenate([keys[:, h // 4 * LANES:(h // 4 + 1) * LANES], key_extra], axis=1),
        lambda b, h: jnp.concatenate(
            [pair_of(queries_t[:, b * LANES:(b + 1) * LANES], h, size), extra1[b, h // 2]], axis=0
        ),
        None,
        lambda b, h: jnp.concatenate([values_t[h * size:(h + 2) * size], ones], axis=0),
        size,
    )

    distant_slot = slot_of(me_lat, (1 - side) * half)

    def send_att(slot, peer):
        group = distant_slot if slot < half else half + (n_lat - 2 - slot) % half
        return pltpu.make_async_remote_copy(
            src_ref=att_out.at[slot * n_lon + partner(peer, 1, n_lon)], dst_ref=att_in.at[group * rows + me_lon], send_sem=s3.at[0],
            recv_sem=r3.at[min(slot // half, 1)], device_id=(peer, lat_at(slot)), device_id_type=MESH,
        )

    def row_done(b, h):
        if h < heads - 2:
            return
        att = jnp.concatenate([row_work.held.pop((b, k)) for k in range(2, heads, 4)], axis=1)
        att_out[b * half * n_lon:(b + 1) * half * n_lon] = att.reshape(half * n_lon, cols, depth).astype(BF16)
        if b == 0:
            pl.semaphore_wait(plane_sem, n_lon - 1)
        for hop in order + [0]:
            for slot in range(b * half, (b + 1) * half):
                if hop or slot < n_lat - 1:
                    send_att(slot, partner(me_lon, hop, n_lon)).start()

    staggered(row_work.stages, [(b, h) for b in (1, 0) for h in range(0, heads, 2)], row_done)
    att_in[pl.ds((n_lat - 1) * rows + me_lon, 1)] = att_out[pl.ds((n_lat - 1) * n_lon + other, 1)]

    for name in ("wo1", "wq2", "wk2", "wv2", "wo2", "wg", "wu", "wd", "gain_lat", "gain_mlp"):
        loads[name].wait()
    wqv2[:depth] = wq2[...].T
    wqv2[depth:] = wv2[...].T
    scale_lat = scales(temp_lat)
    field_all = whole(field_out, field_in, s2.at[0], r2.at[0])
    field_all.wait_recv()

    near_all = whole(att_out.at[pl.ds(0, count // 2 - 1)], att_in.at[pl.ds(0, count // 2 - 1)], s3.at[0], r3.at[1])
    far_all = whole(att_out.at[pl.ds(0, count // 2)], att_in.at[pl.ds(0, count // 2)], s3.at[0], r3.at[0])
    att_all = whole(att_out.at[pl.ds(0, total - 1)], att_in.at[pl.ds(0, total - 1)], s3.at[0], r3.at[0])
    starts = [list(range(cols)), list(range(cols // 2, cols)) + list(range(cols // 2))]

    def by_column(f, values):
        values = values.astype(F32).reshape(LANES, depth)
        parts = []
        for g in range(groups):
            shuffle[groups * f + g] = values[:, g * LANES:(g + 1) * LANES]
            parts.append([shuffle[groups * f + g, pl.ds(c, block, stride=cols), :] for c in starts[f]])
        return jnp.concatenate([jnp.concatenate(part, axis=0) for part in parts], axis=1)

    for f in range(2):
        resid[f * LANES:(f + 1) * LANES] = by_column(f, field_in[f * half:(f + 1) * half])

    firsts, keys2, queries2, turned2, values2 = {}, {}, {}, {}, {}

    def project_columns(f):
        attended = by_column(f, att_in[f * block:(f + 1) * block]).astype(BF16)
        firsts[f] = resid[f * LANES:(f + 1) * LANES] + mm(attended, wo1[...])
        gained = (firsts[f] * gain_lat[...]).astype(BF16)
        factor = root_mean(firsts[f])
        across = jnp.broadcast_to(factor, (LANES, LANES)).T[:1]
        turned = jnp.broadcast_to(halves_turned(factor), (LANES, LANES)).T[:1]
        keys2[f] = (mm(gained, wk2[...]) * factor).astype(BF16)
        both_t = mm_nt(wqv2[...], gained)
        queries2[f] = scaled_t(both_t[:depth], [one * across for one in scale_lat])
        turned2[f] = scaled_t(mm_nt(wqv2[:depth], halves_turned(gained)), [one * turned for one in scale_lat])
        values2[f] = (both_t[depth:] * across).astype(BF16)

    near_all.wait_recv()
    project_columns(1)
    far_all.wait_recv()
    project_columns(0)
    part = LANES // 2
    low = (iota((LANES, LANES), 1) < part).astype(F32).astype(BF16)
    high = (iota((LANES, LANES), 1) >= part).astype(F32).astype(BF16)
    ones = jnp.ones((16, LANES), BF16)

    def column_keys(f, c, g):
        lane = slice(g * LANES, (g + 1) * LANES)
        return jnp.concatenate([keys2[c][:part, lane], keys2[1 - c][part:, lane]], axis=0)

    def column_values(f, c, g):
        row = slice(g * LANES, (g + 1) * LANES)
        return jnp.concatenate([values2[c][row] * low + values2[1 - c][row] * high, ones], axis=0)

    col_work = Quads(
        column_keys,
        lambda f, c, g: side_by_side(queries2[f], turned2[f], c if f == 0 else 1 - c, g, size),
        lambda f, c, g: tables[f, c, g],
        column_values,
        size,
    )
    ff = wg.shape[1]
    step_ff = min(ff, 256)

    def send_upd(slot):
        return pltpu.make_async_remote_copy(
            src_ref=upd_out.at[slot], dst_ref=my_cols(out), send_sem=s4.at[0], recv_sem=r4.at[0],
            device_id=(other, lat_at(slot)), device_id_type=MESH,
        )

    def col_done(f, c, g):
        if c != (1 if f == 0 else 0) or g < groups - 1:
            return
        att = jnp.concatenate(
            [jnp.concatenate([col_work.held.pop((f, k, g)) for g in range(groups)], axis=1)
             for k in ((0, 1) if f == 0 else (1, 0))], axis=0
        )
        second = firsts[f] + mm(att.astype(BF16), wo2[...])
        gained = (second * gain_mlp[...]).astype(BF16)
        factor = root_mean(second)
        for k in range(0, ff, step_ff):
            gate = mm(gained, wg[:, k:k + step_ff])
            upper = mm(gained, wu[:, k:k + step_ff])
            hidden[:, k:k + step_ff] = (gate * upper * (jnp.tanh(gate * (0.5 * factor)) + 1.0)).astype(BF16)
        second = second + (0.5 * factor * factor) * mm(hidden[...], wd[...])
        for i, c in enumerate(starts[f]):
            for g in range(groups):
                shuffle[groups * f + g, pl.ds(c, block, stride=cols), :] = (
                    second[i * block:(i + 1) * block, g * LANES:(g + 1) * LANES]
                )
        updated = jnp.concatenate([shuffle[groups * f + g] for g in range(groups)], axis=1)
        upd_out[f * half:(f + 1) * half] = updated.reshape(half, rows, cols, depth).astype(BF16)
        for slot in range(f * half, (f + 1) * half):
            send_upd(slot).start()

    for f in range(2):
        staggered(
            col_work.stages, [(f, c, g) for c in ((0, 1) if f == 0 else (1, 0)) for g in range(groups)], col_done
        )
    norm_all.wait_send()
    field_all.wait_send()
    att_all.wait_send()
    upd_all = whole(upd_out, upd_out, s4.at[0], r4.at[0])
    upd_all.wait_send()
    upd_all.wait_recv()


def fused_body(
    fields, norm_lon, query_lon, key_lon, value_lon, out_lon, temp_lon, bias_lon,
    norm_lat, query_lat, key_lat, value_lat, out_lat, temp_lat, bias_lat,
    norm_mlp, w_gate, w_up, w_down,
):
    rows, width, depth = fields.shape
    heads = temp_lon.shape[0]
    n_lon, n_lat = lax.axis_size("lon"), lax.axis_size("lat")
    cols = width // n_lat
    nlon = width * n_lon
    total = n_lon * n_lat
    cells = rows * width
    place = np.arange(nlon).reshape(n_lon, n_lat, cols).transpose(1, 0, 2).reshape(nlon)
    turn = place * (2.0 * math.pi / nlon)
    waves = np.stack([np.cos(turn)] * 4 + [np.sin(turn)] * 4, axis=1).astype(np.float32)
    high = waves.astype(jnp.bfloat16).astype(np.float32)
    ktab = np.zeros((nlon, LANES), np.float32)
    ktab[:, :8] = np.where(np.arange(8)[None] % 4 < 2, high, waves - high)
    ktab = ktab.astype(jnp.bfloat16).reshape(n_lat, n_lon * cols, LANES)
    qtab = np.zeros((n_lat, 16, LANES), np.float32)
    qtab[:, :8] = np.tile(waves.reshape(n_lat, LANES // 2, 8).transpose(0, 2, 1), (1, 1, 2))
    hbm = pl.BlockSpec(memory_space=pl.ANY)
    weights = (query_lon, key_lon, value_lon, out_lon, query_lat, key_lat, value_lat, out_lat,
               w_gate, w_up, w_down)
    dma = pltpu.SemaphoreType.DMA
    updated = pl.pallas_call(
        functools.partial(block_kernel, n_lon, n_lat, rows, width, depth, heads),
        out_shape=pltpu.VMEM((rows, width, depth), BF16),
        in_specs=[hbm] * 21,
        out_specs=hbm,
        scratch_shapes=[pltpu.VMEM((rows, width, depth), BF16)]
        + [pltpu.VMEM((1, depth), F32)] * 3
        + [pltpu.VMEM((1, heads), F32)] * 4
        + [pltpu.VMEM(ktab.shape, BF16), pltpu.VMEM(qtab.shape, F32)]
        + [pltpu.VMEM(w.shape, w.dtype) for w in weights]
        + [
            pltpu.VMEM((rows, n_lat, cols, depth), BF16),
            pltpu.VMEM((n_lat, n_lon, cols, depth), BF16),
            pltpu.VMEM((n_lat, rows, cols, depth), BF16),
            pltpu.VMEM((n_lat, rows, cols, depth), BF16),
            pltpu.VMEM((total, cols, depth), BF16),
            pltpu.VMEM((n_lat * rows, cols, depth), BF16),
            pltpu.VMEM((n_lat, rows, cols, depth), BF16),
            pltpu.VMEM((2 * depth, depth), BF16),
            pltpu.VMEM((2 * depth, depth), BF16),
            pltpu.VMEM((2, heads // 2, 16, 2 * LANES), BF16),
            pltpu.VMEM((2, 2, depth // LANES, LANES, 2 * LANES), F32),
            pltpu.VMEM((cells, depth), F32),
            pltpu.VMEM((2 * depth // LANES, LANES, LANES), F32),
            pltpu.VMEM((LANES, w_gate.shape[1]), BF16),
            dma((32,)),
            dma((1,)), dma((1,)),
            dma((1,)), dma((1,)),
            dma((1,)), dma((2,)),
            dma((1,)), dma((1,)),
            pltpu.SemaphoreType.REGULAR((2,)),
            pltpu.SemaphoreType.REGULAR,
        ],
        compiler_params=pltpu.CompilerParams(collective_id=0, has_side_effects=True),
    )(
        fields, norm_lon[None], norm_lat[None], norm_mlp[None], temp_lon[None], bias_lon[None],
        temp_lat[None], bias_lat[None],
        jnp.asarray(ktab), jnp.asarray(qtab), *weights,
    )
    return updated


def fits(rows, width, n_lon, n_lat, heads, depth):
    return (
        rows == n_lon and n_lat % 2 == 0 and width == 8 * n_lat and rows * width == 2 * LANES
        and width * n_lon == 2 * LANES and n_lat == 4 and depth % LANES == 0 and heads * LANES == 4 * depth
    )


def choose(*args):
    rows, width, _ = args[0].shape
    n_lon, n_lat = lax.axis_size("lon"), lax.axis_size("lat")
    if fits(rows, width, n_lon, n_lat, args[6].shape[0], args[0].shape[2]):
        return fused_body(*args)
    return body(*args)


def solution(mesh):
    in_specs = (P("lat", "lon", None),) + (P(),) * 18
    out_specs = P("lat", "lon", None)
    return jax.shard_map(choose, mesh=mesh, in_specs=in_specs, out_specs=out_specs, check_vma=False)
```
